1024 devices in a mesh: face: 8 (over y), tx: 32 (over z, x_hi), ty: 4 (over x_lo, core).
Axes of the slice: x: 8 (x_hi: 4, x_lo: 2; x = x_hi * 2 + x_lo), y: 8, z: 8, core: 2. Of those that a mesh axis runs over, the one named last changes fastest.
Arguments:
- probes: float32 [2, 4, 8, 6, 256, 256], P(None, None, 'face', None, 'tx', 'ty'), may hold values from -6 to 6
- background_wind: float32 [2, 8, 6, 256, 256], P(None, 'face', None, 'tx', 'ty'), may hold values from -6 to 6
- layer_mass: float32 [8, 6, 256, 256], P('face', None, 'tx', 'ty'), may hold values from 0.5 to 2
- trajectory_heat_factor: float32 [8, 6, 256, 256], P('face', None, 'tx', 'ty'), may hold values from 0.3 to 3
- spread: float32 [4, 8, 6, 256, 256], P(None, 'face', None, 'tx', 'ty'), may hold values from 0.5 to 2
- inverse_misfit_variance: float32 [4, 8, 6, 256, 256], P(None, 'face', None, 'tx', 'ty'), may hold values from 0.25 to 4
- face_links: int32 [6, 4, 7], replicated, may hold values from -1 to 5, as said below
Outputs:
- applied: float32 [2, 4, 8, 6, 256, 256], P(None, None, 'face', None, 'tx', 'ty')
The draws below stay inside these ranges and needn't reach their ends.
Inputs may be any that keep to these rules, and one draw needn't show every extreme that they name: `face_links`: the table describes the six panels of a cube, each with a right-handed frame: for panel f and edge e, the panel across it, the edge of that panel which touches f, whether the index along the shared edge runs the other way, and the matrix of entries -1, 0, 1 that carries vector components from that panel's frame into the frame of f.
All inputs are finite; a program needn't handle non-finite values.
Results may differ from the reference program's by a relative error of at most 0.00002.
Values sent between devices are 32-bit elements; how exact they have to be, the bound alone decides.
No kernel may reach another device: no remote copies, remote signals or barrier semaphores. Data moves between devices by JAX's collectives and lax.ppermute only.
A program may use at most 64 MiB of HBM per device.

```python
import math
import jax
import jax.numpy as jnp

PROBES = 2
LEV = 8
SIDE = 256


def draw_face_links(key, part):
    centre = jnp.array([[1, 0, 0], [-1, 0, 0], [0, 1, 0], [0, -1, 0], [0, 0, 1], [0, 0, -1]], jnp.int32)
    across = jnp.array([[0, 1, 0], [0, 0, 1], [0, 0, 1], [1, 0, 0], [1, 0, 0], [0, 1, 0]], jnp.int32)
    upward = jnp.array([[0, 0, 1], [0, 1, 0], [1, 0, 0], [0, 0, 1], [0, 1, 0], [1, 0, 0]], jnp.int32)
    order = jax.random.permutation(jax.random.fold_in(key, 11), 6)
    quarter = jax.random.randint(jax.random.fold_in(key, 12), (6,), 0, 4)
    centre = centre[order]
    across = across[order]
    upward = upward[order]
    turned = quarter[:, None]
    new_across = jnp.where(turned == 0, across, jnp.where(turned == 1, upward, jnp.where(turned == 2, -across, -upward)))
    new_upward = jnp.where(turned == 0, upward, jnp.where(turned == 1, -across, jnp.where(turned == 2, -upward, across)))
    across = new_across
    upward = new_upward
    outward = jnp.stack([-across, across, -upward, upward], axis=1)
    along_edge = jnp.stack([upward, upward, across, across], axis=1)
    hits = jnp.all(outward[:, :, None, :] == centre[None, None, :, :], axis=-1)
    neighbour = jnp.sum(hits.astype(jnp.int32) * jnp.arange(6, dtype=jnp.int32), axis=-1)
    far_out = outward[neighbour]
    back_hits = jnp.all(far_out == centre[:, None, None, :], axis=-1).astype(jnp.int32)
    far_edge = jnp.sum(back_hits * jnp.arange(4, dtype=jnp.int32), axis=-1)
    far_along = jnp.sum(back_hits[..., None] * along_edge[neighbour], axis=2)
    reverse = (jnp.sum(along_edge * far_along, axis=-1) < 0).astype(jnp.int32)
    near_centre = centre[:, None, :]
    folding = near_centre + outward

    def carried(vectors):
        return vectors - jnp.sum(vectors * near_centre, axis=-1, keepdims=True) * folding

    def projected(vectors, basis):
        return jnp.sum(vectors * basis, axis=-1)
    far_across = carried(across[neighbour])
    far_upward = carried(upward[neighbour])
    near_across = across[:, None, :]
    near_upward = upward[:, None, :]
    table = jnp.stack([neighbour, far_edge, reverse, projected(far_across, near_across), projected(far_upward, near_across), projected(far_across, near_upward), projected(far_upward, near_upward)], axis=-1)
    return table.astype(jnp.int32)


def steps_of(key, extent, split, smallest, top_value):
    level = 1.0
    for position, blocks in split:
        steps = jax.random.uniform(jax.random.fold_in(jax.random.fold_in(key, 6), position), (blocks,), jnp.float32, smallest / len(split), top_value / len(split))
        level = level * jnp.repeat(jnp.exp(steps), extent[position] // blocks).reshape((-1,) + (1,) * (len(extent) - 1 - position))
    return level


def gaussian(stream_key, shape, scale, reach, cuts=(), held_as=jnp.bfloat16):
    values = jax.random.normal(stream_key, shape, jnp.float32) * scale
    if len(cuts) > 0:
        values = steps_of(stream_key, shape, cuts, -0.22, 0.18) * values
    return jnp.clip(values, min=-reach, max=reach).astype(held_as)


def setup_inputs(seed: int = 0) -> dict:
    splits = jax.random.split(jax.random.key(seed), 8)
    probes = gaussian(splits[0], (PROBES, 4, LEV, 6, SIDE, SIDE), 1.0, 6.0, ((2, 8), (4, 32), (5, 4)), jnp.float32)
    background_wind = gaussian(splits[1], (2, LEV, 6, SIDE, SIDE), 1.0, 6.0, ((1, 8), (3, 32), (4, 4)), jnp.float32)
    layer_mass = jnp.clip(jnp.exp(math.log(2.0) - 1.3862944 * jax.random.uniform(splits[2], (LEV, 6, SIDE, SIDE), jnp.float32) ** steps_of(splits[2], (LEV, 6, SIDE, SIDE), ((0, 8), (2, 32), (3, 4)), -0.2, 0.2)), 0.5, 2.0)
    trajectory_heat_factor = jnp.clip(jnp.exp(math.log(3.0) - 2.3025851 * jax.random.uniform(splits[3], (LEV, 6, SIDE, SIDE), jnp.float32) ** steps_of(splits[3], (LEV, 6, SIDE, SIDE), ((0, 8), (2, 32), (3, 4)), -0.2, 0.2)), 0.3, 3.0)
    spread = jnp.clip(jnp.exp(math.log(2.0) - 1.3862944 * jax.random.uniform(splits[4], (4, LEV, 6, SIDE, SIDE), jnp.float32) ** steps_of(splits[4], (4, LEV, 6, SIDE, SIDE), ((1, 8), (3, 32), (4, 4)), -0.2, 0.2)), 0.5, 2.0)
    inverse_misfit_variance = jnp.clip(jnp.exp(math.log(4.0) - 2.7725887 * jax.random.uniform(splits[5], (4, LEV, 6, SIDE, SIDE), jnp.float32) ** steps_of(splits[5], (4, LEV, 6, SIDE, SIDE), ((1, 8), (3, 32), (4, 4)), -0.2, 0.2)), 0.25, 4.0)
    face_links = draw_face_links(jax.random.fold_in(splits[7], 71), 0)
    return dict(probes=probes, background_wind=background_wind, layer_mass=layer_mass, trajectory_heat_factor=trajectory_heat_factor, spread=spread, inverse_misfit_variance=inverse_misfit_variance, face_links=face_links)


time_increment = 0.3
forward_layout = (('vector', 0), ('vector', 2), ('scalar', 4), ('scalar', 5))

def carry_pair(leading, trailing, entries):
    return (entries[0] * leading + entries[1] * trailing, entries[2] * leading + entries[3] * trailing)

def rotate_edge(edge_strip, matrix_codes, layout):
    matrix = matrix_codes.astype(edge_strip.dtype)
    entries = [matrix[:, column].reshape(1, 1, 6, 1) for column in range(4)]
    channels = [edge_strip[number] for number in range(edge_strip.shape[0])]
    for species, offset in layout:
        if species == 'vector':
            channels[offset], channels[offset + 1] = carry_pair(channels[offset], channels[offset + 1], entries)
        elif species == 'tensor':
            channels[offset], channels[offset + 1] = carry_pair(channels[offset], channels[offset + 1], entries)
            channels[offset + 2], channels[offset + 3] = carry_pair(channels[offset + 2], channels[offset + 3], entries)
            channels[offset], channels[offset + 2] = carry_pair(channels[offset], channels[offset + 2], entries)
            channels[offset + 1], channels[offset + 3] = carry_pair(channels[offset + 1], channels[offset + 3], entries)
    return jnp.stack(channels)

def orient(edge_rows, face_links, side, layout):
    source_face = face_links[:, side, 0]
    source_edge = face_links[:, side, 1]
    chosen = edge_rows[:, :, :, source_face, source_edge, :]
    flipped = (face_links[:, side, 2] == 1).reshape(1, 1, 1, 6, 1)
    chosen = jnp.where(flipped, chosen[..., ::-1], chosen)
    return rotate_edge(chosen, face_links[:, side, 3:7], layout)

def extend(fields, face_links, layout):
    edge_rows = jnp.stack([fields[..., 0, :], fields[..., -1, :], fields[..., :, 0], fields[..., :, -1]], axis=4)
    padded = jnp.pad(fields, ((0, 0), (0, 0), (0, 0), (0, 0), (1, 1), (1, 1)))
    padded = padded.at[..., 0, 1:-1].set(orient(edge_rows, face_links, 0, layout))
    padded = padded.at[..., -1, 1:-1].set(orient(edge_rows, face_links, 1, layout))
    padded = padded.at[..., 1:-1, 0].set(orient(edge_rows, face_links, 2, layout))
    padded = padded.at[..., 1:-1, -1].set(orient(edge_rows, face_links, 3, layout))
    return padded

def slopes(padded):
    east_slope_derivative = 0.5 * (padded[..., 2:, 1:-1] - padded[..., :-2, 1:-1])
    north_slope_derivative = 0.5 * (padded[..., 1:-1, 2:] - padded[..., 1:-1, :-2])
    return (east_slope_derivative, north_slope_derivative)

def tangent(normalised_state_array, background_wind, layer_mass, trajectory_heat_factor, face_links):
    west_east_wind_part, south_north_wind_speed, sheet_depth_state, sheet_warmth_state = (normalised_state_array[:, 0], normalised_state_array[:, 1], normalised_state_array[:, 2], normalised_state_array[:, 3])
    east_wind_speed, north_wind_speed = (background_wind[0], background_wind[1])
    ground_barometric_load = jnp.cumsum(sheet_depth_state, axis=1)
    gravity_potential_level = sheet_warmth_state + trajectory_heat_factor * ground_barometric_load
    east_mass_transport = east_wind_speed * sheet_depth_state + layer_mass * west_east_wind_part
    north_mass_transport = north_wind_speed * sheet_depth_state + layer_mass * south_north_wind_speed
    joined_state_arrays = jnp.stack([west_east_wind_part, south_north_wind_speed, east_mass_transport, north_mass_transport, sheet_warmth_state, gravity_potential_level])
    east_slope_derivative, north_slope_derivative = slopes(extend(joined_state_arrays, face_links, forward_layout))
    west_east_wind_after = west_east_wind_part - time_increment * (east_slope_derivative[5] + east_wind_speed * east_slope_derivative[0] + north_wind_speed * north_slope_derivative[0])
    south_north_wind_after = south_north_wind_speed - time_increment * (north_slope_derivative[5] + east_wind_speed * east_slope_derivative[1] + north_wind_speed * north_slope_derivative[1])
    depth_after_update = sheet_depth_state - time_increment * (east_slope_derivative[2] + north_slope_derivative[3])
    warmth_after_update = sheet_warmth_state - time_increment * (east_wind_speed * east_slope_derivative[4] + north_wind_speed * north_slope_derivative[4])
    return jnp.stack([west_east_wind_after, south_north_wind_after, depth_after_update, warmth_after_update], axis=1)

def reference(probes, background_wind, layer_mass, trajectory_heat_factor, spread, inverse_misfit_variance, face_links):
    normalised_state_array = spread[None] * probes

    def linear_step(perturbed):
        return tangent(perturbed, background_wind, layer_mass, trajectory_heat_factor, face_links)
    model_image, pullback = jax.vjp(linear_step, normalised_state_array)
    adjoint_out, = pullback(inverse_misfit_variance[None] * model_image)
    return probes + spread[None] * adjoint_out
```

```python
import functools

import jax
import jax.numpy as jnp
import numpy as np
from jax import lax
from jax.experimental import pallas as pl
from jax.experimental.pallas import tpu as pltpu
from jax.sharding import PartitionSpec as P

dt = 0.3
PROBES = 2
FORWARD = ("zonal", "meridional", "flux_x", "flux_y", "temp", "geo")
FORWARD_X = {
    "geo": {"geo": (0, 0)},
    "zonal": {"zonal": (1, 0), "meridional": (2, 0)},
    "meridional": {"zonal": (3, 0), "meridional": (4, 0)},
    "flux_x": {"flux_x": (1, 0), "flux_y": (2, 0)},
    "temp": {"temp": (0, 0)},
}
FORWARD_Y = {
    "geo": {"geo": (0, 0)},
    "zonal": {"zonal": (1, 0), "meridional": (2, 0)},
    "meridional": {"zonal": (3, 0), "meridional": (4, 0)},
    "flux_y": {"flux_x": (3, 0), "flux_y": (4, 0)},
    "temp": {"temp": (0, 0)},
}
ADJOINT = ("ez", "em", "nz", "nm", "z", "m", "t", "eh", "nh")
ADJOINT_X = {
    "ez": {"ez": (1, 1), "em": (1, 2), "nz": (2, 1), "nm": (2, 2)},
    "em": {"ez": (1, 3), "em": (1, 4), "nz": (2, 3), "nm": (2, 4)},
    "z": {"z": (1, 0), "m": (2, 0)},
    "t": {"t": (0, 0)},
    "eh": {"eh": (1, 0), "nh": (2, 0)},
}
ADJOINT_Y = {
    "nz": {"ez": (3, 1), "em": (3, 2), "nz": (4, 1), "nm": (4, 2)},
    "nm": {"ez": (3, 3), "em": (3, 4), "nz": (4, 3), "nm": (4, 4)},
    "m": {"z": (3, 0), "m": (4, 0)},
    "t": {"t": (0, 0)},
    "nh": {"eh": (3, 0), "nh": (4, 0)},
}
ROWS = 56
STRIP = 16 + ROWS


def source_index(unit, panel):
    return (panel % 2) * 64 + unit * 3 + panel // 2


def target_index(unit, panel):
    return (panel % 2) * 32 + unit * 3 + panel // 2


def codes_of(sources, x_targets, y_targets):
    codes = np.full((5, 128, 64), -1.0, np.float32)
    for d, targets in enumerate((x_targets, y_targets)):
        for t, (_, terms) in enumerate(targets.items()):
            for name, (i, j) in terms.items():
                s = sources.index(name)
                for probe in range(PROBES):
                    for n in range(6):
                        for f in range(6):
                            r = source_index(s * PROBES + probe, n)
                            c = target_index(t * PROBES + probe, f)
                            codes[2 * d, r, c] = i
                            codes[2 * d + 1, r, c] = j
    for u in range(len(sources) * PROBES):
        for n in range(6):
            codes[4, source_index(u, n), :] = n
    return codes


def picks_of(sources, y_targets):
    picks = np.zeros((128, 64), np.float32)
    for t, name in enumerate(y_targets):
        for probe in range(PROBES):
            for f in range(6):
                picks[
                    source_index(sources.index(name) * PROBES + probe, f),
                    target_index(t * PROBES + probe, f),
                ] = 1.0
    return picks


TABLES = {
    "forward": (FORWARD, FORWARD_X, FORWARD_Y),
    "adjoint": (ADJOINT, ADJOINT_X, ADJOINT_Y),
}


def dot(a, b, contract=(1, 0)):
    return lax.dot_general(
        a,
        b,
        (((contract[0],), (contract[1],)), ((), ())),
        precision=lax.Precision.HIGHEST,
        preferred_element_type=jnp.float32,
    )


def reversal(size):
    row = lax.broadcasted_iota(jnp.int32, (size, size), 0)
    column = lax.broadcasted_iota(jnp.int32, (size, size), 1)
    return (row + column == size - 1).astype(jnp.float32)


def identity(size):
    row = lax.broadcasted_iota(jnp.int32, (size, size), 0)
    column = lax.broadcasted_iota(jnp.int32, (size, size), 1)
    return (row == column).astype(jnp.float32)


def lanes(shape):
    return lax.broadcasted_iota(jnp.int32, shape, len(shape) - 1)


def joined(even, odd):
    return jnp.concatenate([even, odd], axis=1)


def pair(ref, index, pp):
    return joined(ref[(*index, 2 * pp)], ref[(*index, 2 * pp + 1)])


def link_lanes(links, edge, item):
    lane = lanes((1, 64))
    within = jnp.where(lane >= 32, lane - 32, lane)
    third = within - 3 * ((within * 43) // 128)
    out = jnp.zeros((1, 64), jnp.float32)
    for f in range(6):
        value = links[f * 28 + edge * 7 + item].astype(jnp.float32)
        here = (third == f // 2) & ((lane >= 32) == (f % 2 == 1))
        out = jnp.where(here, value, out)
    return out


def coefficients(links, edge, code_a, code_b, panel):
    one = jnp.ones((1, 64), jnp.float32)
    entries = [one] + [link_lanes(links, edge, 3 + k) for k in range(4)]
    a = jnp.zeros(code_a.shape, jnp.float32)
    b = jnp.zeros(code_a.shape, jnp.float32)
    for k in range(5):
        a = jnp.where(code_a == k, entries[k], a)
        b = jnp.where(code_b == k, entries[k], b)
    return jnp.where(panel == link_lanes(links, edge, 0), a * b, 0.0)


def put_strips(planes, out_ref, tile_row):
    lane = lanes((8, 128))
    south = jnp.zeros((8, 128), jnp.float32)
    north = jnp.zeros((8, 128), jnp.float32)
    rows = []
    for a, plane in enumerate(planes):
        here = (lane == a) | (lane == a + 64)
        south = jnp.where(here, plane if a == 0 else pltpu.roll(plane, a, 1), south)
        shift = (a - 63) % 128
        north = jnp.where(here, plane if shift == 0 else pltpu.roll(plane, shift, 1), north)
        rows.append(jnp.where(tile_row == 0, plane[0:1], plane[7:8]))
    out_ref[0:8] = south
    out_ref[8:16] = north
    rows.append(jnp.zeros((ROWS - len(rows), 128), jnp.float32))
    out_ref[16:STRIP] = jnp.concatenate(rows, axis=0)


def put_outer_rows(planes, top_ref, bottom_ref):
    spare = [jnp.zeros((32 - len(planes), 128), jnp.float32)]
    top_ref[...] = jnp.concatenate([p[0:1] for p in planes] + spare, axis=0)
    bottom_ref[...] = jnp.concatenate([p[7:8] for p in planes] + spare, axis=0)


def slopes_x(plane, b, west, east):
    row = lax.broadcasted_iota(jnp.int32, (8, 128), 0)
    after = jnp.where(row == 7, east[b : b + 1], pltpu.roll(plane, 7, 0))
    before = jnp.where(row == 0, west[b : b + 1], pltpu.roll(plane, 1, 0))
    return 0.5 * (after - before)


def slopes_y(plane, b, south, north):
    lane = lanes((8, 128))
    low = (lane == 0) | (lane == 64)
    high = (lane == 63) | (lane == 127)
    from_south = south if b == 0 else pltpu.roll(south, 128 - b, 1)
    after = jnp.where(high, pltpu.roll(north, 63 - b, 1), pltpu.roll(plane, 127, 1))
    before = jnp.where(low, from_south, pltpu.roll(plane, 1, 1))
    return 0.5 * (after - before)


def thickness_kernel(slots, probes, spread, out):
    for probe in range(PROBES):
        for pp in range(3):
            value = pair(spread, (2, 0), pp) * pair(probes, (probe, 2, 0), pp)
            for k in range(slots):
                out[k, (probe * 3 + pp) * 8 : (probe * 3 + pp) * 8 + 8] = value


def fields_kernel(
    level_count, place, probes, spread, wind, mass, heat, totals, fields, strips, top, bottom
):
    level = place[0]
    planes = {}
    for pp in range(3):
        east = pair(wind, (0, 0), pp)
        north = pair(wind, (1, 0), pp)
        mass_here = pair(mass, (0,), pp)
        heat_here = pair(heat, (0,), pp)
        for probe in range(PROBES):
            scaled = [
                pair(spread, (c, 0), pp) * pair(probes, (probe, c, 0), pp) for c in range(4)
            ]
            zonal, meridional, thickness, temp = scaled
            at = (probe * 3 + pp) * 8
            pressure = thickness
            for k in range(level_count - 1):
                pressure = pressure + jnp.where(k < level, totals[k, at : at + 8], 0.0)
            planes["zonal", probe, pp] = zonal
            planes["meridional", probe, pp] = meridional
            planes["flux_x", probe, pp] = east * thickness + mass_here * zonal
            planes["flux_y", probe, pp] = north * thickness + mass_here * meridional
            planes["temp", probe, pp] = temp
            planes["geo", probe, pp] = temp + heat_here * pressure
    ordered = [planes[n, pr, pp] for n in FORWARD for pr in range(PROBES) for pp in range(3)]
    for a, plane in enumerate(ordered):
        fields[a] = plane
    put_strips(ordered, strips, place[1])
    put_outer_rows(
        [planes[n, pr, pp] for n in FORWARD_X for pr in range(PROBES) for pp in range(3)],
        top,
        bottom,
    )


def route_kernel(
    nt, nq, place, links, gathered, top, bottom, codes, picks, slots, swap_a, swap_b, local, halos
):
    tile_row, tile_column = place[1], place[2]
    is_first, is_last = tile_row == 0, tile_row == nt - 1
    line = jnp.where(is_first, 0, 1)
    line_f = line.astype(jnp.float32)
    column_edge = jnp.where(tile_column == 0, 2, 3)
    panel = codes[4]
    c0 = coefficients(links, 0, codes[0], codes[1], panel)
    c1 = coefficients(links, 1, codes[0], codes[1], panel)
    cc = coefficients(links, column_edge, codes[2], codes[3], panel)

    def masks(edge, source):
        far = link_lanes(links, edge, 1)
        flip = link_lanes(links, edge, 2)
        here = far == source
        return (
            jnp.where(here & (flip != 1.0), 1.0, 0.0),
            jnp.where(here & (flip == 1.0), 1.0, 0.0),
        )

    back64 = reversal(64)
    empty = jnp.zeros((64 - ROWS, 64), jnp.float32)

    def segment(q):
        packed = gathered[q, 16:STRIP]
        return jnp.concatenate([packed[:, 0:64], empty, packed[:, 64:128], empty], axis=0)

    on_boundary = jnp.where(is_first | is_last, 1.0, 0.0)
    plain_c, turned_c = masks(column_edge, line_f)
    across = [dot(segment(q), cc, (0, 0)) for q in range(nq)]
    pieces = []
    for q in range(nq):
        pieces.append(
            on_boundary
            * (across[q] * plain_c + dot(back64, across[nq - 1 - q] * turned_c))
        )
    low_column, high_column = gathered[0, 0:8], gathered[nq - 1, 8:16]
    low_plain, low_turned = masks(column_edge, 2.0)
    high_plain, high_turned = masks(column_edge, 3.0)
    low_c, high_c = dot(low_column, cc), dot(high_column, cc)
    straight = low_c * low_plain + high_c * high_plain
    flipped = dot(reversal(8), low_c * low_turned + high_c * high_turned)
    to_rows = []
    for edge, c in ((0, c0), (1, c1)):
        far = link_lanes(links, edge, 1)
        to_rows.append(
            dot(low_column, c) * jnp.where(far == 2.0, 1.0, 0.0)
            + dot(high_column, c) * jnp.where(far == 3.0, 1.0, 0.0)
        )
    for t in range(nt):
        q, at = t // 8, (t % 8) * 8
        left = pieces[q][at : at + 8]
        left = left + jnp.where(tile_row == t, straight, 0.0)
        left = left + jnp.where(tile_row == nt - 1 - t, flipped, 0.0)
        slots[t] = joined(left, to_rows[1] if t == nt - 1 else to_rows[0])

    mine, mirrored = gathered[tile_column, 16:STRIP], gathered[nq - 1 - tile_column, 16:STRIP]
    mine = jnp.concatenate([mine[:, 0:64], empty, mine[:, 64:128], empty], axis=0)
    mirrored = jnp.concatenate([mirrored[:, 0:64], empty, mirrored[:, 64:128], empty], axis=0)
    by_row = []
    for edge, c in ((0, c0), (1, c1)):
        plain, turned = masks(edge, line_f)
        by_row.append(
            dot(c * plain, mine, (0, 0)) + dot(dot(c * turned, mirrored, (0, 0)), back64)
        )
    by_row = [joined(z[0:32], z[32:64]) for z in by_row]
    local[...] = jnp.where(is_first, by_row[0], by_row[1])
    to_lower = jnp.where(is_first, by_row[1], top[...])
    to_upper = jnp.where(is_last, by_row[0], bottom[...])
    even = lax.rem(tile_row, 2) == 0
    swap_a[...] = jnp.where(even, to_upper, to_lower)
    swap_b[...] = jnp.where(even, to_lower, to_upper)

    below = gathered[jnp.maximum(tile_column - 1, 0), 8:16]
    above = gathered[jnp.minimum(tile_column + 1, nq - 1), 0:8]
    halos[0:8] = jnp.where(tile_column > 0, dot(below, picks[...]), 0.0)
    halos[8:16] = jnp.where(tile_column < nq - 1, dot(above, picks[...]), 0.0)


def outer_values(nt, nq, place, links, arrived, swapped_a, swapped_b, local, halos):
    tile_row, tile_column = place[1], place[2]
    is_first, is_last = tile_row == 0, tile_row == nt - 1
    column = arrived[0]
    for t in range(1, nt):
        column = column + arrived[t]
    column = column[:, 0:64]
    south = halos[0:8] + jnp.where(tile_column == 0, column, 0.0)
    north = halos[8:16] + jnp.where(tile_column == nq - 1, column, 0.0)
    lane = lanes((8, 128))

    def spread_out(narrow):
        wide = joined(narrow, narrow)
        return jnp.where(lane < 32, wide, pltpu.roll(wide, 32, 1))

    mine = arrived[pl.ds(tile_column * 8, 8)].reshape(64, 128)[:, 64:128]
    mirrored = arrived[pl.ds((nq - 1 - tile_column) * 8, 8)].reshape(64, 128)[:, 64:128]
    flip = link_lanes(links, jnp.where(is_first, 0, 1), 2)
    row = dot(jnp.where(flip != 1.0, mine, 0.0), identity(64), (0, 0)) + dot(
        jnp.where(flip == 1.0, mirrored, 0.0), reversal(64), (0, 0)
    )
    row = joined(row[0:32], row[32:64]) + local[...]
    even = lax.rem(tile_row, 2) == 0
    west = jnp.where(even, swapped_b[...], swapped_a[...]) + jnp.where(is_first, row, 0.0)
    east = jnp.where(even, swapped_a[...], swapped_b[...]) + jnp.where(is_last, row, 0.0)
    return west, east, spread_out(south), spread_out(north)


def image_kernel(
    nt,
    nq,
    place,
    links,
    arrived,
    swapped_a,
    swapped_b,
    local,
    halos,
    fields,
    probes,
    spread,
    wind,
    misfit,
    costs,
    strips,
    top,
    bottom,
):
    west, east, south, north = outer_values(
        nt, nq, place, links, arrived, swapped_a, swapped_b, local, halos
    )
    planes = {}
    for pp in range(3):
        u = pair(wind, (0, 0), pp)
        v = pair(wind, (1, 0), pp)
        for probe in range(PROBES):
            field = lambda n: fields[(FORWARD.index(n) * PROBES + probe) * 3 + pp]
            at = lambda n, t: (list(t).index(n) * PROBES + probe) * 3 + pp
            dx = {n: slopes_x(field(n), at(n, FORWARD_X), west, east) for n in FORWARD_X}
            dy = {n: slopes_y(field(n), at(n, FORWARD_Y), south, north) for n in FORWARD_Y}
            thickness = pair(spread, (2, 0), pp) * pair(probes, (probe, 2, 0), pp)
            z = field("zonal") - dt * (dx["geo"] + u * dx["zonal"] + v * dy["zonal"])
            m = field("meridional") - dt * (
                dy["geo"] + u * dx["meridional"] + v * dy["meridional"]
            )
            t = thickness - dt * (dx["flux_x"] + dy["flux_y"])
            h = field("temp") - dt * (u * dx["temp"] + v * dy["temp"])
            z, m, t, h = (pair(misfit, (c, 0), pp) * w for c, w in enumerate((z, m, t, h)))
            for c, w in enumerate((z, m, t, h)):
                costs[(c * PROBES + probe) * 3 + pp] = w
            made = (u * z, u * m, v * z, v * m, z, m, t, u * h, v * h)
            for n, w in zip(ADJOINT, made):
                planes[n, probe, pp] = w
    put_strips(
        [planes[n, pr, pp] for n in ADJOINT for pr in range(PROBES) for pp in range(3)],
        strips,
        place[1],
    )
    put_outer_rows(
        [planes[n, pr, pp] for n in ADJOINT_X for pr in range(PROBES) for pp in range(3)],
        top,
        bottom,
    )


def adjoint_kernel(
    nt,
    nq,
    levels,
    place,
    links,
    arrived,
    swapped_a,
    swapped_b,
    local,
    halos,
    costs,
    wind,
    mass,
    heat,
    backs,
    loads,
):
    west, east, south, north = outer_values(
        nt, nq, place, links, arrived, swapped_a, swapped_b, local, halos
    )
    for pp in range(3):
        u = pair(wind, (0, 0), pp)
        v = pair(wind, (1, 0), pp)
        mass_here = pair(mass, (0,), pp)
        heat_here = pair(heat, (0,), pp)
        for probe in range(PROBES):
            z, m, t, h = (costs[(c * PROBES + probe) * 3 + pp] for c in range(4))
            field = dict(
                zip(ADJOINT, (u * z, u * m, v * z, v * m, z, m, t, u * h, v * h))
            )
            at = lambda n, k: (list(k).index(n) * PROBES + probe) * 3 + pp
            dx = {n: slopes_x(field[n], at(n, ADJOINT_X), west, east) for n in ADJOINT_X}
            dy = {n: slopes_y(field[n], at(n, ADJOINT_Y), south, north) for n in ADJOINT_Y}
            geo_back = dt * (dx["z"] + dy["m"])
            flux_x_back = dt * dx["t"]
            flux_y_back = dt * dy["t"]
            out = (
                z + dt * (dx["ez"] + dy["nz"]) + mass_here * flux_x_back,
                m + dt * (dx["em"] + dy["nm"]) + mass_here * flux_y_back,
                t + u * flux_x_back + v * flux_y_back,
                h + dt * (dx["eh"] + dy["nh"]) + geo_back,
            )
            for c, w in enumerate(out):
                backs[(c * PROBES + probe) * 3 + pp] = w
            load = heat_here * geo_back
            for k in range(levels):
                loads[k, (probe * 3 + pp) * 8 : (probe * 3 + pp) * 8 + 8] = load


def final_kernel(level_count, place, probes, spread, backs, loads, out):
    level = place[0]
    for probe in range(PROBES):
        for pp in range(3):
            at = (probe * 3 + pp) * 8
            load = jnp.zeros((8, 128), jnp.float32)
            for k in range(level_count):
                load = load + jnp.where(k >= level, loads[k, at : at + 8], 0.0)
            for c in range(4):
                back = backs[(c * PROBES + probe) * 3 + pp]
                if c == 2:
                    back = back + load
                for side in range(2):
                    part = back[:, 64 * side : 64 * side + 64]
                    p = 2 * pp + side
                    out[probe, c, 0, p] = probes[probe, c, 0, p] + spread[c, 0, p] * part


SMEM = pl.BlockSpec(memory_space=pltpu.SMEM)
VMEM = pl.BlockSpec(memory_space=pltpu.VMEM)
INTERPRET = False


def call(kernel, name, small, operands, shapes):
    shapes = [jax.ShapeDtypeStruct(s, jnp.float32) for s in shapes]
    return pl.pallas_call(
        kernel,
        name=name,
        out_shape=shapes,
        in_specs=[SMEM] * len(small) + [VMEM] * len(operands),
        out_specs=[VMEM] * len(shapes),
        interpret=INTERPRET,
    )(*small, *operands)


def exchange(kind, nt, nq, place, links, strips, top, bottom):
    sources, x_targets, y_targets = TABLES[kind]
    codes = jnp.asarray(codes_of(sources, x_targets, y_targets))
    picks = jnp.asarray(picks_of(sources, y_targets))
    gathered = lax.all_gather(strips, "ty", axis=0)
    slots, swap_a, swap_b, local, halos = call(
        functools.partial(route_kernel, nt, nq),
        "route_" + kind,
        (place, links),
        (gathered, top, bottom, codes, picks),
        ((nt, 8, 128), (32, 128), (32, 128), (32, 128), (16, 64)),
    )
    near = [(i, i ^ 1) for i in range(nt)]
    wrapped = [(i, (i + 1 if i % 2 else i - 1) % nt) for i in range(nt)]
    swapped_a = lax.ppermute(swap_a, "tx", near)
    swapped_b = lax.ppermute(swap_b, "tx", wrapped)
    arrived = lax.all_to_all(slots, "tx", 0, 0, tiled=True)
    return arrived, swapped_a, swapped_b, local, halos


def body(probes, wind, mass, heat, spread, misfit, face_links):
    nf, nt, nq = (lax.axis_size(a) for a in ("face", "tx", "ty"))
    links = face_links.reshape(-1)
    index = lax.broadcasted_iota(jnp.int32, (3,), 0)
    place = jnp.where(
        index == 0,
        lax.axis_index("face"),
        jnp.where(index == 1, lax.axis_index("tx"), lax.axis_index("ty")),
    )
    (sent,) = call(
        functools.partial(thickness_kernel, nf),
        "thickness",
        (),
        (probes, spread),
        ((nf, 48, 128),),
    )
    totals = lax.all_to_all(sent, "face", 0, 0, tiled=True)
    fields, strips, top, bottom = call(
        functools.partial(fields_kernel, nf),
        "fields",
        (place,),
        (probes, spread, wind, mass, heat, totals),
        ((36, 8, 128), (STRIP, 128), (32, 128), (32, 128)),
    )
    outer = exchange("forward", nt, nq, place, links, strips, top, bottom)
    costs, strips, top, bottom = call(
        functools.partial(image_kernel, nt, nq),
        "image",
        (place, links),
        (*outer, fields, probes, spread, wind, misfit),
        ((24, 8, 128), (STRIP, 128), (32, 128), (32, 128)),
    )
    outer = exchange("adjoint", nt, nq, place, links, strips, top, bottom)
    backs, loads = call(
        functools.partial(adjoint_kernel, nt, nq, nf),
        "adjoint",
        (place, links),
        (*outer, costs, wind, mass, heat),
        ((24, 8, 128), (nf, 48, 128)),
    )
    loads = lax.all_to_all(loads, "face", 0, 0, tiled=True)
    (applied,) = call(
        functools.partial(final_kernel, nf),
        "final",
        (place,),
        (probes, spread, backs, loads),
        (probes.shape,),
    )
    return applied


def solution(mesh):
    return jax.shard_map(
        body,
        mesh=mesh,
        in_specs=(
            P(None, None, "face", None, "tx", "ty"),
            P(None, "face", None, "tx", "ty"),
            P("face", None, "tx", "ty"),
            P("face", None, "tx", "ty"),
            P(None, "face", None, "tx", "ty"),
            P(None, "face", None, "tx", "ty"),
            P(),
        ),
        out_specs=P(None, None, "face", None, "tx", "ty"),
        check_vma=False,
    )
```

```python
import functools

import jax
import jax.numpy as jnp
import numpy as np
from jax import lax
from jax.experimental import pallas as pl
from jax.experimental.pallas import tpu as pltpu
from jax.sharding import PartitionSpec as P

dt = 0.3
PROBES = 2
FORWARD = ("zonal", "meridional", "flux_x", "flux_y", "temp", "geo")
FORWARD_X = {
    "geo": {"geo": (0, 0)},
    "zonal": {"zonal": (1, 0), "meridional": (2, 0)},
    "meridional": {"zonal": (3, 0), "meridional": (4, 0)},
    "flux_x": {"flux_x": (1, 0), "flux_y": (2, 0)},
    "temp": {"temp": (0, 0)},
}
FORWARD_Y = {
    "geo": {"geo": (0, 0)},
    "zonal": {"zonal": (1, 0), "meridional": (2, 0)},
    "meridional": {"zonal": (3, 0), "meridional": (4, 0)},
    "flux_y": {"flux_x": (3, 0), "flux_y": (4, 0)},
    "temp": {"temp": (0, 0)},
}
ADJOINT = ("ez", "em", "nz", "nm", "z", "m", "t", "eh", "nh")
ADJOINT_X = {
    "ez": {"ez": (1, 1), "em": (1, 2), "nz": (2, 1), "nm": (2, 2)},
    "em": {"ez": (1, 3), "em": (1, 4), "nz": (2, 3), "nm": (2, 4)},
    "z": {"z": (1, 0), "m": (2, 0)},
    "t": {"t": (0, 0)},
    "eh": {"eh": (1, 0), "nh": (2, 0)},
}
ADJOINT_Y = {
    "nz": {"ez": (3, 1), "em": (3, 2), "nz": (4, 1), "nm": (4, 2)},
    "nm": {"ez": (3, 3), "em": (3, 4), "nz": (4, 3), "nm": (4, 4)},
    "m": {"z": (3, 0), "m": (4, 0)},
    "t": {"t": (0, 0)},
    "nh": {"eh": (3, 0), "nh": (4, 0)},
}
ROWS = 56
STRIP = 16 + ROWS


def source_index(unit, panel):
    return (panel % 2) * 64 + unit * 3 + panel // 2


def target_index(unit, panel):
    return (panel % 2) * 32 + unit * 3 + panel // 2


def codes_of(sources, x_targets, y_targets):
    codes = np.full((5, 128, 64), -1.0, np.float32)
    for d, targets in enumerate((x_targets, y_targets)):
        for t, (_, terms) in enumerate(targets.items()):
            for name, (i, j) in terms.items():
                s = sources.index(name)
                for probe in range(PROBES):
                    for n in range(6):
                        for f in range(6):
                            r = source_index(s * PROBES + probe, n)
                            c = target_index(t * PROBES + probe, f)
                            codes[2 * d, r, c] = i
                            codes[2 * d + 1, r, c] = j
    for u in range(len(sources) * PROBES):
        for n in range(6):
            codes[4, source_index(u, n), :] = n
    return codes


def picks_of(sources, y_targets):
    picks = np.zeros((128, 64), np.float32)
    for t, name in enumerate(y_targets):
        for probe in range(PROBES):
            for f in range(6):
                picks[
                    source_index(sources.index(name) * PROBES + probe, f),
                    target_index(t * PROBES + probe, f),
                ] = 1.0
    return picks


TABLES = {
    "forward": (FORWARD, FORWARD_X, FORWARD_Y),
    "adjoint": (ADJOINT, ADJOINT_X, ADJOINT_Y),
}


def dot(a, b, contract=(1, 0)):
    return lax.dot_general(
        a,
        b,
        (((contract[0],), (contract[1],)), ((), ())),
        precision=lax.Precision.HIGHEST,
        preferred_element_type=jnp.float32,
    )


def reversal(size):
    row = lax.broadcasted_iota(jnp.int32, (size, size), 0)
    column = lax.broadcasted_iota(jnp.int32, (size, size), 1)
    return (row + column == size - 1).astype(jnp.float32)


def identity(size):
    row = lax.broadcasted_iota(jnp.int32, (size, size), 0)
    column = lax.broadcasted_iota(jnp.int32, (size, size), 1)
    return (row == column).astype(jnp.float32)


def lanes(shape):
    return lax.broadcasted_iota(jnp.int32, shape, len(shape) - 1)


def joined(even, odd):
    return jnp.concatenate([even, odd], axis=1)


def pair(ref, index, pp):
    return joined(ref[(*index, 2 * pp)], ref[(*index, 2 * pp + 1)])


def link_lanes(links, edge, item):
    lane = lanes((1, 64))
    within = jnp.where(lane >= 32, lane - 32, lane)
    third = within - 3 * ((within * 43) // 128)
    out = jnp.zeros((1, 64), jnp.float32)
    for f in range(6):
        value = links[f * 28 + edge * 7 + item].astype(jnp.float32)
        here = (third == f // 2) & ((lane >= 32) == (f % 2 == 1))
        out = jnp.where(here, value, out)
    return out


def coefficients(links, edge, code_a, code_b, panel):
    one = jnp.ones((1, 64), jnp.float32)
    entries = [one] + [link_lanes(links, edge, 3 + k) for k in range(4)]
    a = jnp.zeros(code_a.shape, jnp.float32)
    b = jnp.zeros(code_a.shape, jnp.float32)
    for k in range(5):
        a = jnp.where(code_a == k, entries[k], a)
        b = jnp.where(code_b == k, entries[k], b)
    return jnp.where(panel == link_lanes(links, edge, 0), a * b, 0.0)


def put_strips(planes, out_ref, tile_row):
    lane = lanes((8, 128))
    south = jnp.zeros((8, 128), jnp.float32)
    north = jnp.zeros((8, 128), jnp.float32)
    rows = []
    for a, plane in enumerate(planes):
        here = (lane == a) | (lane == a + 64)
        south = jnp.where(here, plane if a == 0 else pltpu.roll(plane, a, 1), south)
        shift = (a - 63) % 128
        north = jnp.where(here, plane if shift == 0 else pltpu.roll(plane, shift, 1), north)
        rows.append(jnp.where(tile_row == 0, plane[0:1], plane[7:8]))
    out_ref[0:8] = south
    out_ref[8:16] = north
    rows.append(jnp.zeros((ROWS - len(rows), 128), jnp.float32))
    out_ref[16:STRIP] = jnp.concatenate(rows, axis=0)


def put_outer_rows(planes, top_ref, bottom_ref):
    spare = [jnp.zeros((32 - len(planes), 128), jnp.float32)]
    top_ref[...] = jnp.concatenate([p[0:1] for p in planes] + spare, axis=0)
    bottom_ref[...] = jnp.concatenate([p[7:8] for p in planes] + spare, axis=0)


def slopes_x(plane, b, west, east):
    row = lax.broadcasted_iota(jnp.int32, (8, 128), 0)
    after = jnp.where(row == 7, east[b : b + 1], pltpu.roll(plane, 7, 0))
    before = jnp.where(row == 0, west[b : b + 1], pltpu.roll(plane, 1, 0))
    return 0.5 * (after - before)


def slopes_y(plane, b, south, north):
    lane = lanes((8, 128))
    low = (lane == 0) | (lane == 64)
    high = (lane == 63) | (lane == 127)
    from_south = south if b == 0 else pltpu.roll(south, 128 - b, 1)
    after = jnp.where(high, pltpu.roll(north, 63 - b, 1), pltpu.roll(plane, 127, 1))
    before = jnp.where(low, from_south, pltpu.roll(plane, 1, 1))
    return 0.5 * (after - before)


def thickness_kernel(slots, probes, spread, out):
    for probe in range(PROBES):
        for pp in range(3):
            value = pair(spread, (2, 0), pp) * pair(probes, (probe, 2, 0), pp)
            for k in range(slots):
                out[k, (probe * 3 + pp) * 8 : (probe * 3 + pp) * 8 + 8] = value


def fields_kernel(
    level_count, place, probes, spread, wind, mass, heat, totals, fields, strips, top, bottom
):
    level = place[0]
    planes = {}
    for pp in range(3):
        east = pair(wind, (0, 0), pp)
        north = pair(wind, (1, 0), pp)
        mass_here = pair(mass, (0,), pp)
        heat_here = pair(heat, (0,), pp)
        for probe in range(PROBES):
            scaled = [
                pair(spread, (c, 0), pp) * pair(probes, (probe, c, 0), pp) for c in range(4)
            ]
            zonal, meridional, thickness, temp = scaled
            at = (probe * 3 + pp) * 8
            pressure = thickness
            for k in range(level_count - 1):
                pressure = pressure + jnp.where(k < level, totals[k, at : at + 8], 0.0)
            planes["zonal", probe, pp] = zonal
            planes["meridional", probe, pp] = meridional
            planes["flux_x", probe, pp] = east * thickness + mass_here * zonal
            planes["flux_y", probe, pp] = north * thickness + mass_here * meridional
            planes["temp", probe, pp] = temp
            planes["geo", probe, pp] = temp + heat_here * pressure
    ordered = [planes[n, pr, pp] for n in FORWARD for pr in range(PROBES) for pp in range(3)]
    for a, plane in enumerate(ordered):
        fields[a] = plane
    put_strips(ordered, strips, place[1])
    put_outer_rows(
        [planes[n, pr, pp] for n in FORWARD_X for pr in range(PROBES) for pp in range(3)],
        top,
        bottom,
    )


def route_kernel(
    nt, nq, place, links, gathered, top, bottom, codes, picks, slots, swap_a, swap_b, local, halos
):
    tile_row, tile_column = place[1], place[2]
    is_first, is_last = tile_row == 0, tile_row == nt - 1
    line = jnp.where(is_first, 0, 1)
    line_f = line.astype(jnp.float32)
    column_edge = jnp.where(tile_column == 0, 2, 3)
    panel = codes[4]
    c0 = coefficients(links, 0, codes[0], codes[1], panel)
    c1 = coefficients(links, 1, codes[0], codes[1], panel)
    cc = coefficients(links, column_edge, codes[2], codes[3], panel)

    def masks(edge, source):
        far = link_lanes(links, edge, 1)
        flip = link_lanes(links, edge, 2)
        here = far == source
        return (
            jnp.where(here & (flip != 1.0), 1.0, 0.0),
            jnp.where(here & (flip == 1.0), 1.0, 0.0),
        )

    back64 = reversal(64)
    empty = jnp.zeros((64 - ROWS, 64), jnp.float32)

    def segment(q):
        packed = gathered[q, 16:STRIP]
        return jnp.concatenate([packed[:, 0:64], empty, packed[:, 64:128], empty], axis=0)

    on_boundary = jnp.where(is_first | is_last, 1.0, 0.0)
    plain_c, turned_c = masks(column_edge, line_f)
    across = [dot(segment(q), cc, (0, 0)) for q in range(nq)]
    pieces = []
    for q in range(nq):
        pieces.append(
            on_boundary
            * (across[q] * plain_c + dot(back64, across[nq - 1 - q] * turned_c))
        )
    low_column, high_column = gathered[0, 0:8], gathered[nq - 1, 8:16]
    low_plain, low_turned = masks(column_edge, 2.0)
    high_plain, high_turned = masks(column_edge, 3.0)
    low_c, high_c = dot(low_column, cc), dot(high_column, cc)
    straight = low_c * low_plain + high_c * high_plain
    flipped = dot(reversal(8), low_c * low_turned + high_c * high_turned)
    to_rows = []
    for edge, c in ((0, c0), (1, c1)):
        far = link_lanes(links, edge, 1)
        to_rows.append(
            dot(low_column, c) * jnp.where(far == 2.0, 1.0, 0.0)
            + dot(high_column, c) * jnp.where(far == 3.0, 1.0, 0.0)
        )
    for t in range(nt):
        q, at = t // 8, (t % 8) * 8
        left = pieces[q][at : at + 8]
        left = left + jnp.where(tile_row == t, straight, 0.0)
        left = left + jnp.where(tile_row == nt - 1 - t, flipped, 0.0)
        slots[t] = joined(left, to_rows[1] if t == nt - 1 else to_rows[0])

    mine, mirrored = gathered[tile_column, 16:STRIP], gathered[nq - 1 - tile_column, 16:STRIP]
    mine = jnp.concatenate([mine[:, 0:64], empty, mine[:, 64:128], empty], axis=0)
    mirrored = jnp.concatenate([mirrored[:, 0:64], empty, mirrored[:, 64:128], empty], axis=0)
    by_row = []
    for edge, c in ((0, c0), (1, c1)):
        plain, turned = masks(edge, line_f)
        by_row.append(
            dot(c * plain, mine, (0, 0)) + dot(dot(c * turned, mirrored, (0, 0)), back64)
        )
    by_row = [joined(z[0:32], z[32:64]) for z in by_row]
    local[...] = jnp.where(is_first, by_row[0], by_row[1])
    to_lower = jnp.where(is_first, by_row[1], top[...])
    to_upper = jnp.where(is_last, by_row[0], bottom[...])
    even = lax.rem(tile_row, 2) == 0
    swap_a[...] = jnp.where(even, to_upper, to_lower)
    swap_b[...] = jnp.where(even, to_lower, to_upper)

    below = gathered[jnp.maximum(tile_column - 1, 0), 8:16]
    above = gathered[jnp.minimum(tile_column + 1, nq - 1), 0:8]
    halos[0:8] = jnp.where(tile_column > 0, dot(below, picks[...]), 0.0)
    halos[8:16] = jnp.where(tile_column < nq - 1, dot(above, picks[...]), 0.0)


def outer_values(nt, nq, place, links, arrived, swapped_a, swapped_b, local, halos):
    tile_row, tile_column = place[1], place[2]
    is_first, is_last = tile_row == 0, tile_row == nt - 1
    column = arrived[0]
    for t in range(1, nt):
        column = column + arrived[t]
    column = column[:, 0:64]
    south = halos[0:8] + jnp.where(tile_column == 0, column, 0.0)
    north = halos[8:16] + jnp.where(tile_column == nq - 1, column, 0.0)
    lane = lanes((8, 128))

    def spread_out(narrow):
        wide = joined(narrow, narrow)
        return jnp.where(lane < 32, wide, pltpu.roll(wide, 32, 1))

    mine = arrived[pl.ds(tile_column * 8, 8)].reshape(64, 128)[:, 64:128]
    mirrored = arrived[pl.ds((nq - 1 - tile_column) * 8, 8)].reshape(64, 128)[:, 64:128]
    flip = link_lanes(links, jnp.where(is_first, 0, 1), 2)
    row = dot(jnp.where(flip != 1.0, mine, 0.0), identity(64), (0, 0)) + dot(
        jnp.where(flip == 1.0, mirrored, 0.0), reversal(64), (0, 0)
    )
    row = joined(row[0:32], row[32:64]) + local[...]
    even = lax.rem(tile_row, 2) == 0
    west = jnp.where(even, swapped_b[...], swapped_a[...]) + jnp.where(is_first, row, 0.0)
    east = jnp.where(even, swapped_a[...], swapped_b[...]) + jnp.where(is_last, row, 0.0)
    return west, east, spread_out(south), spread_out(north)


def image_kernel(
    nt,
    nq,
    place,
    links,
    arrived,
    swapped_a,
    swapped_b,
    local,
    halos,
    fields,
    probes,
    spread,
    wind,
    misfit,
    costs,
    strips,
    top,
    bottom,
):
    west, east, south, north = outer_values(
        nt, nq, place, links, arrived, swapped_a, swapped_b, local, halos
    )
    planes = {}
    for pp in range(3):
        u = pair(wind, (0, 0), pp)
        v = pair(wind, (1, 0), pp)
        for probe in range(PROBES):
            field = lambda n: fields[(FORWARD.index(n) * PROBES + probe) * 3 + pp]
            at = lambda n, t: (list(t).index(n) * PROBES + probe) * 3 + pp
            dx = {n: slopes_x(field(n), at(n, FORWARD_X), west, east) for n in FORWARD_X}
            dy = {n: slopes_y(field(n), at(n, FORWARD_Y), south, north) for n in FORWARD_Y}
            thickness = pair(spread, (2, 0), pp) * pair(probes, (probe, 2, 0), pp)
            z = field("zonal") - dt * (dx["geo"] + u * dx["zonal"] + v * dy["zonal"])
            m = field("meridional") - dt * (
                dy["geo"] + u * dx["meridional"] + v * dy["meridional"]
            )
            t = thickness - dt * (dx["flux_x"] + dy["flux_y"])
            h = field("temp") - dt * (u * dx["temp"] + v * dy["temp"])
            z, m, t, h = (pair(misfit, (c, 0), pp) * w for c, w in enumerate((z, m, t, h)))
            for c, w in enumerate((z, m, t, h)):
                costs[(c * PROBES + probe) * 3 + pp] = w
            made = (u * z, u * m, v * z, v * m, z, m, t, u * h, v * h)
            for n, w in zip(ADJOINT, made):
                planes[n, probe, pp] = w
    put_strips(
        [planes[n, pr, pp] for n in ADJOINT for pr in range(PROBES) for pp in range(3)],
        strips,
        place[1],
    )
    put_outer_rows(
        [planes[n, pr, pp] for n in ADJOINT_X for pr in range(PROBES) for pp in range(3)],
        top,
        bottom,
    )


def adjoint_kernel(
    nt,
    nq,
    levels,
    place,
    links,
    arrived,
    swapped_a,
    swapped_b,
    local,
    halos,
    costs,
    wind,
    mass,
    heat,
    backs,
    loads,
):
    west, east, south, north = outer_values(
        nt, nq, place, links, arrived, swapped_a, swapped_b, local, halos
    )
    for pp in range(3):
        u = pair(wind, (0, 0), pp)
        v = pair(wind, (1, 0), pp)
        mass_here = pair(mass, (0,), pp)
        heat_here = pair(heat, (0,), pp)
        for probe in range(PROBES):
            z, m, t, h = (costs[(c * PROBES + probe) * 3 + pp] for c in range(4))
            field = dict(
                zip(ADJOINT, (u * z, u * m, v * z, v * m, z, m, t, u * h, v * h))
            )
            at = lambda n, k: (list(k).index(n) * PROBES + probe) * 3 + pp
            dx = {n: slopes_x(field[n], at(n, ADJOINT_X), west, east) for n in ADJOINT_X}
            dy = {n: slopes_y(field[n], at(n, ADJOINT_Y), south, north) for n in ADJOINT_Y}
            geo_back = dt * (dx["z"] + dy["m"])
            flux_x_back = dt * dx["t"]
            flux_y_back = dt * dy["t"]
            out = (
                z + dt * (dx["ez"] + dy["nz"]) + mass_here * flux_x_back,
                m + dt * (dx["em"] + dy["nm"]) + mass_here * flux_y_back,
                t + u * flux_x_back + v * flux_y_back,
                h + dt * (dx["eh"] + dy["nh"]) + geo_back,
            )
            for c, w in enumerate(out):
                backs[(c * PROBES + probe) * 3 + pp] = w
            load = heat_here * geo_back
            for k in range(levels):
                loads[k, (probe * 3 + pp) * 8 : (probe * 3 + pp) * 8 + 8] = load


def final_kernel(level_count, place, probes, spread, backs, loads, out):
    level = place[0]
    for probe in range(PROBES):
        for pp in range(3):
            at = (probe * 3 + pp) * 8
            load = jnp.zeros((8, 128), jnp.float32)
            for k in range(level_count):
                load = load + jnp.where(k >= level, loads[k, at : at + 8], 0.0)
            for c in range(4):
                back = backs[(c * PROBES + probe) * 3 + pp]
                if c == 2:
                    back = back + load
                for side in range(2):
                    part = back[:, 64 * side : 64 * side + 64]
                    p = 2 * pp + side
                    out[probe, c, 0, p] = probes[probe, c, 0, p] + spread[c, 0, p] * part


SMEM = pl.BlockSpec(memory_space=pltpu.SMEM)
VMEM = pl.BlockSpec(memory_space=pltpu.VMEM)
INTERPRET = False
GRANT = 8 << 20


def call(kernel, small, operands, shapes):
    shapes = [jax.ShapeDtypeStruct(s, jnp.float32) for s in shapes]
    return pl.pallas_call(
        kernel,
        out_shape=shapes,
        in_specs=[SMEM] * len(small) + [VMEM] * len(operands),
        out_specs=[VMEM] * len(shapes),
        compiler_params=pltpu.CompilerParams(vmem_limit_bytes=GRANT),
        interpret=INTERPRET,
    )(*small, *operands)


def exchange(kind, nt, nq, place, links, strips, top, bottom):
    sources, x_targets, y_targets = TABLES[kind]
    codes = jnp.asarray(codes_of(sources, x_targets, y_targets))
    picks = jnp.asarray(picks_of(sources, y_targets))
    gathered = lax.all_gather(strips, "ty", axis=0)
    slots, swap_a, swap_b, local, halos = call(
        functools.partial(route_kernel, nt, nq),
        (place, links),
        (gathered, top, bottom, codes, picks),
        ((nt, 8, 128), (32, 128), (32, 128), (32, 128), (16, 64)),
    )
    near = [(i, i ^ 1) for i in range(nt)]
    wrapped = [(i, (i + 1 if i % 2 else i - 1) % nt) for i in range(nt)]
    swapped_a = lax.ppermute(swap_a, "tx", near)
    swapped_b = lax.ppermute(swap_b, "tx", wrapped)
    arrived = lax.all_to_all(slots, "tx", 0, 0, tiled=True)
    return arrived, swapped_a, swapped_b, local, halos


def body(probes, wind, mass, heat, spread, misfit, face_links):
    nf, nt, nq = (lax.axis_size(a) for a in ("face", "tx", "ty"))
    links = face_links.reshape(-1)
    index = lax.broadcasted_iota(jnp.int32, (3,), 0)
    place = jnp.where(
        index == 0,
        lax.axis_index("face"),
        jnp.where(index == 1, lax.axis_index("tx"), lax.axis_index("ty")),
    )
    (sent,) = call(functools.partial(thickness_kernel, nf), (), (probes, spread), ((nf, 48, 128),))
    totals = lax.all_to_all(sent, "face", 0, 0, tiled=True)
    fields, strips, top, bottom = call(
        functools.partial(fields_kernel, nf),
        (place,),
        (probes, spread, wind, mass, heat, totals),
        ((36, 8, 128), (STRIP, 128), (32, 128), (32, 128)),
    )
    outer = exchange("forward", nt, nq, place, links, strips, top, bottom)
    costs, strips, top, bottom = call(
        functools.partial(image_kernel, nt, nq),
        (place, links),
        (*outer, fields, probes, spread, wind, misfit),
        ((24, 8, 128), (STRIP, 128), (32, 128), (32, 128)),
    )
    outer = exchange("adjoint", nt, nq, place, links, strips, top, bottom)
    backs, loads = call(
        functools.partial(adjoint_kernel, nt, nq, nf),
        (place, links),
        (*outer, costs, wind, mass, heat),
        ((24, 8, 128), (nf, 48, 128)),
    )
    loads = lax.all_to_all(loads, "face", 0, 0, tiled=True)
    (applied,) = call(
        functools.partial(final_kernel, nf),
        (place,),
        (probes, spread, backs, loads),
        (probes.shape,),
    )
    return applied


def solution(mesh):
    return jax.shard_map(
        body,
        mesh=mesh,
        in_specs=(
            P(None, None, "face", None, "tx", "ty"),
            P(None, "face", None, "tx", "ty"),
            P("face", None, "tx", "ty"),
            P("face", None, "tx", "ty"),
            P(None, "face", None, "tx", "ty"),
            P(None, "face", None, "tx", "ty"),
            P(),
        ),
        out_specs=P(None, None, "face", None, "tx", "ty"),
        check_vma=False,
    )
```

```python
import functools

import jax
import jax.numpy as jnp
import numpy as np
from jax import lax
from jax.experimental import pallas as pl
from jax.experimental.pallas import tpu as pltpu
from jax.sharding import PartitionSpec as P

dt = 0.3
PROBES = 2
FORWARD = ("zonal", "meridional", "flux_x", "flux_y", "temp", "geo")
FORWARD_X = {
    "geo": {"geo": (0, 0)},
    "zonal": {"zonal": (1, 0), "meridional": (2, 0)},
    "meridional": {"zonal": (3, 0), "meridional": (4, 0)},
    "flux_x": {"flux_x": (1, 0), "flux_y": (2, 0)},
    "temp": {"temp": (0, 0)},
}
FORWARD_Y = {
    "geo": {"geo": (0, 0)},
    "zonal": {"zonal": (1, 0), "meridional": (2, 0)},
    "meridional": {"zonal": (3, 0), "meridional": (4, 0)},
    "flux_y": {"flux_x": (3, 0), "flux_y": (4, 0)},
    "temp": {"temp": (0, 0)},
}
ADJOINT = ("ez", "em", "nz", "nm", "z", "m", "t", "eh", "nh")
ADJOINT_X = {
    "ez": {"ez": (1, 1), "em": (1, 2), "nz": (2, 1), "nm": (2, 2)},
    "em": {"ez": (1, 3), "em": (1, 4), "nz": (2, 3), "nm": (2, 4)},
    "z": {"z": (1, 0), "m": (2, 0)},
    "t": {"t": (0, 0)},
    "eh": {"eh": (1, 0), "nh": (2, 0)},
}
ADJOINT_Y = {
    "nz": {"ez": (3, 1), "em": (3, 2), "nz": (4, 1), "nm": (4, 2)},
    "nm": {"ez": (3, 3), "em": (3, 4), "nz": (4, 3), "nm": (4, 4)},
    "m": {"z": (3, 0), "m": (4, 0)},
    "t": {"t": (0, 0)},
    "nh": {"eh": (3, 0), "nh": (4, 0)},
}
ROWS = 56
STRIP = 16 + ROWS


def source_index(unit, panel):
    return (panel % 2) * 64 + unit * 3 + panel // 2


def target_index(unit, panel):
    return (panel % 2) * 32 + unit * 3 + panel // 2


def codes_of(sources, x_targets, y_targets):
    codes = np.full((5, 128, 64), -1.0, np.float32)
    for d, targets in enumerate((x_targets, y_targets)):
        for t, (_, terms) in enumerate(targets.items()):
            for name, (i, j) in terms.items():
                s = sources.index(name)
                for probe in range(PROBES):
                    for n in range(6):
                        for f in range(6):
                            r = source_index(s * PROBES + probe, n)
                            c = target_index(t * PROBES + probe, f)
                            codes[2 * d, r, c] = i
                            codes[2 * d + 1, r, c] = j
    for u in range(len(sources) * PROBES):
        for n in range(6):
            codes[4, source_index(u, n), :] = n
    return codes


def picks_of(sources, y_targets):
    picks = np.zeros((128, 64), np.float32)
    for t, name in enumerate(y_targets):
        for probe in range(PROBES):
            for f in range(6):
                picks[
                    source_index(sources.index(name) * PROBES + probe, f),
                    target_index(t * PROBES + probe, f),
                ] = 1.0
    return picks


TABLES = {
    "forward": (FORWARD, FORWARD_X, FORWARD_Y),
    "adjoint": (ADJOINT, ADJOINT_X, ADJOINT_Y),
}


def parts(data):
    high = data.astype(jnp.bfloat16)
    rest = data - high.astype(jnp.float32)
    middle = rest.astype(jnp.bfloat16)
    low = (rest - middle.astype(jnp.float32)).astype(jnp.bfloat16)
    return high, middle, low


def product(a, b, contract):
    return lax.dot_general(
        a,
        b,
        (((contract[0],), (contract[1],)), ((), ())),
        preferred_element_type=jnp.float32,
    )


def moved(data, choice, contract=(1, 0)):
    high, middle, low = (product(d, choice, contract) for d in data)
    return (high + middle) + low


def chosen(choice, data, contract=(1, 0)):
    high, middle, low = (product(choice, d, contract) for d in data)
    return (high + middle) + low


def reversal(size):
    row = lax.broadcasted_iota(jnp.int32, (size, size), 0)
    column = lax.broadcasted_iota(jnp.int32, (size, size), 1)
    return (row + column == size - 1).astype(jnp.float32).astype(jnp.bfloat16)


def identity(size):
    row = lax.broadcasted_iota(jnp.int32, (size, size), 0)
    column = lax.broadcasted_iota(jnp.int32, (size, size), 1)
    return (row == column).astype(jnp.float32).astype(jnp.bfloat16)


def lanes(shape):
    return lax.broadcasted_iota(jnp.int32, shape, len(shape) - 1)


def joined(even, odd):
    return jnp.concatenate([even, odd], axis=1)


def joined_all(pieces):
    return jnp.concatenate(pieces, axis=1)


def pair(ref, index, pp):
    return joined(ref[(*index, 2 * pp)], ref[(*index, 2 * pp + 1)])


def link_lanes(links, edge, item):
    lane = lanes((1, 64))
    within = jnp.where(lane >= 32, lane - 32, lane)
    third = within - 3 * ((within * 43) // 128)
    out = jnp.zeros((1, 64), jnp.float32)
    for f in range(6):
        value = links[f, edge, item].astype(jnp.float32)
        here = (third == f // 2) & ((lane >= 32) == (f % 2 == 1))
        out = jnp.where(here, value, out)
    return out


def coefficients(links, edge, code_a, code_b, panel):
    one = jnp.ones((1, 64), jnp.float32)
    entries = [one] + [link_lanes(links, edge, 3 + k) for k in range(4)]
    a = jnp.zeros(code_a.shape, jnp.float32)
    b = jnp.zeros(code_a.shape, jnp.float32)
    for k in range(5):
        a = jnp.where(code_a == k, entries[k], a)
        b = jnp.where(code_b == k, entries[k], b)
    return jnp.where(panel == link_lanes(links, edge, 0), a * b, 0.0)


def put_strips(planes, out_ref, tile_row):
    lane = lanes((8, 128))
    south = jnp.zeros((8, 128), jnp.float32)
    north = jnp.zeros((8, 128), jnp.float32)
    rows = []
    for a, plane in enumerate(planes):
        here = (lane == a) | (lane == a + 64)
        south = jnp.where(here, plane if a == 0 else pltpu.roll(plane, a, 1), south)
        shift = (a - 63) % 128
        north = jnp.where(here, plane if shift == 0 else pltpu.roll(plane, shift, 1), north)
        rows.append(jnp.where(tile_row == 0, plane[0:1], plane[7:8]))
    out_ref[0:8] = south
    out_ref[8:16] = north
    rows.append(jnp.zeros((ROWS - len(rows), 128), jnp.float32))
    out_ref[16:STRIP] = jnp.concatenate(rows, axis=0)


def put_outer_rows(planes, top_ref, bottom_ref):
    spare = [jnp.zeros((32 - len(planes), 128), jnp.float32)]
    top_ref[...] = jnp.concatenate([p[0:1] for p in planes] + spare, axis=0)
    bottom_ref[...] = jnp.concatenate([p[7:8] for p in planes] + spare, axis=0)


def slopes_x(plane, b, west, east):
    row = lax.broadcasted_iota(jnp.int32, (8, 128), 0)
    after = jnp.where(row == 7, east[b : b + 1], pltpu.roll(plane, 7, 0))
    before = jnp.where(row == 0, west[b : b + 1], pltpu.roll(plane, 1, 0))
    return 0.5 * (after - before)


def slopes_y(plane, b, south, north):
    lane = lanes((8, 128))
    low = (lane == 0) | (lane == 64)
    high = (lane == 63) | (lane == 127)
    from_south = south if b == 0 else pltpu.roll(south, 128 - b, 1)
    after = jnp.where(high, pltpu.roll(north, 63 - b, 1), pltpu.roll(plane, 127, 1))
    before = jnp.where(low, from_south, pltpu.roll(plane, 1, 1))
    return 0.5 * (after - before)


def thickness_kernel(slots, probes, spread, out):
    for probe in range(PROBES):
        for pp in range(3):
            value = pair(spread, (0, 0), pp) * pair(probes, (probe, 0, 0), pp)
            for k in range(slots):
                out[k, (probe * 3 + pp) * 8 : (probe * 3 + pp) * 8 + 8] = value


def fields_kernel(
    level_count, probes, spread, wind, mass, heat, totals, fields, strips, top, bottom
):
    level, tile_row = lax.axis_index("face"), lax.axis_index("tx")
    planes = {}
    for pp in range(3):
        east = pair(wind, (0, 0), pp)
        north = pair(wind, (1, 0), pp)
        mass_here = pair(mass, (0,), pp)
        heat_here = pair(heat, (0,), pp)
        for probe in range(PROBES):
            scaled = [
                pair(spread, (c, 0), pp) * pair(probes, (probe, c, 0), pp) for c in range(4)
            ]
            zonal, meridional, thickness, temp = scaled
            at = (probe * 3 + pp) * 8
            pressure = thickness
            for k in range(level_count - 1):
                pressure = pressure + jnp.where(k < level, totals[k, at : at + 8], 0.0)
            planes["zonal", probe, pp] = zonal
            planes["meridional", probe, pp] = meridional
            planes["flux_x", probe, pp] = east * thickness + mass_here * zonal
            planes["flux_y", probe, pp] = north * thickness + mass_here * meridional
            planes["temp", probe, pp] = temp
            planes["geo", probe, pp] = temp + heat_here * pressure
    ordered = [planes[n, pr, pp] for n in FORWARD for pr in range(PROBES) for pp in range(3)]
    for a, plane in enumerate(ordered):
        fields[a] = plane
    put_strips(ordered, strips, tile_row)
    put_outer_rows(
        [planes[n, pr, pp] for n in FORWARD_X for pr in range(PROBES) for pp in range(3)],
        top,
        bottom,
    )


def route_kernel(nt, nq, links, gathered, top, bottom, codes, picks, slots, local, halos):
    tile_row, tile_column = lax.axis_index("tx"), lax.axis_index("ty")
    is_first, is_last = tile_row == 0, tile_row == nt - 1
    line_f = jnp.where(is_first, 0.0, 1.0)
    column_edge = jnp.where(tile_column == 0, 2, 3)
    panel = codes[4]
    c0 = coefficients(links, 0, codes[0], codes[1], panel)
    c1 = coefficients(links, 1, codes[0], codes[1], panel)
    cc = coefficients(links, column_edge, codes[2], codes[3], panel)
    ends = joined(c0, c1).astype(jnp.bfloat16)
    cc = cc.astype(jnp.bfloat16)

    def masks(edge, source):
        far = link_lanes(links, edge, 1)
        flip = link_lanes(links, edge, 2)
        here = far == source
        return (
            jnp.where(here & (flip != 1.0), 1.0, 0.0),
            jnp.where(here & (flip == 1.0), 1.0, 0.0),
        )

    back64 = reversal(64)
    empty = jnp.zeros((64 - ROWS, 64), jnp.float32)

    def segment(q):
        packed = gathered[q, 16:STRIP]
        return parts(
            jnp.concatenate([packed[:, 0:64], empty, packed[:, 64:128], empty], axis=0)
        )

    on_boundary = jnp.where(is_first | is_last, 1.0, 0.0)
    plain_c, turned_c = masks(column_edge, line_f)
    across = [moved(segment(q), cc, (0, 0)) * on_boundary for q in range(nq)]
    turned = joined_all([a * turned_c for a in across])
    turned = chosen(back64, parts(turned))
    pieces = [
        across[q] * plain_c + turned[:, 64 * (nq - 1 - q) : 64 * (nq - q)] for q in range(nq)
    ]
    columns = parts(jnp.concatenate([gathered[0, 0:8], gathered[nq - 1, 8:16]], axis=0))
    low_plain, low_turned = masks(column_edge, 2.0)
    high_plain, high_turned = masks(column_edge, 3.0)
    to_columns = moved(columns, cc)
    low_c, high_c = to_columns[0:8], to_columns[8:16]
    straight = low_c * low_plain + high_c * high_plain
    flipped = chosen(reversal(8), parts(low_c * low_turned + high_c * high_turned))
    to_rows = moved(columns, ends)
    far = joined(link_lanes(links, 0, 1), link_lanes(links, 1, 1))
    to_rows = to_rows[0:8] * jnp.where(far == 2.0, 1.0, 0.0) + to_rows[8:16] * jnp.where(
        far == 3.0, 1.0, 0.0
    )
    to_rows = [to_rows[:, 0:64], to_rows[:, 64:128]]
    for t in range(nt):
        q, at = t // 8, (t % 8) * 8
        left = pieces[q][at : at + 8]
        left = left + jnp.where(tile_row == t, straight, 0.0)
        left = left + jnp.where(tile_row == nt - 1 - t, flipped, 0.0)
        slots[t, 0:8] = joined(left, to_rows[1] if t == nt - 1 else to_rows[0])

    plain0, turned0 = masks(0, line_f)
    plain1, turned1 = masks(1, line_f)
    plain = (joined(c0, c1) * joined(plain0, plain1)).astype(jnp.bfloat16)
    mirror = (joined(c0, c1) * joined(turned0, turned1)).astype(jnp.bfloat16)
    by_row = chosen(plain, segment(tile_column), (0, 0))
    by_row = by_row + moved(
        parts(chosen(mirror, segment(nq - 1 - tile_column), (0, 0))), back64
    )
    by_row = [joined(by_row[k : k + 32], by_row[k + 32 : k + 64]) for k in (0, 64)]
    local[...] = jnp.where(is_first, by_row[0], by_row[1])
    slots[lax.rem(tile_row + nt - 1, nt), 8:40] = jnp.where(is_first, by_row[1], top[...])
    slots[lax.rem(tile_row + 1, nt), 8:40] = jnp.where(is_last, by_row[0], bottom[...])

    below = gathered[jnp.maximum(tile_column - 1, 0), 8:16]
    above = gathered[jnp.minimum(tile_column + 1, nq - 1), 0:8]
    near = moved(parts(jnp.concatenate([below, above], axis=0)), picks[...].astype(jnp.bfloat16))
    halos[0:8] = jnp.where(tile_column > 0, near[0:8], 0.0)
    halos[8:16] = jnp.where(tile_column < nq - 1, near[8:16], 0.0)


def outer_values(nt, nq, links, arrived, local, halos):
    tile_row, tile_column = lax.axis_index("tx"), lax.axis_index("ty")
    is_first, is_last = tile_row == 0, tile_row == nt - 1
    column = arrived[0, 0:8]
    for t in range(1, nt):
        column = column + arrived[t, 0:8]
    column = column[:, 0:64]
    south = halos[0:8] + jnp.where(tile_column == 0, column, 0.0)
    north = halos[8:16] + jnp.where(tile_column == nq - 1, column, 0.0)
    lane = lanes((8, 128))

    def spread_out(narrow):
        wide = joined(narrow, narrow)
        return jnp.where(lane < 32, wide, pltpu.roll(wide, 32, 1))

    mine = arrived[pl.ds(tile_column * 8, 8), 0:8].reshape(64, 128)[:, 64:128]
    mirrored = arrived[pl.ds((nq - 1 - tile_column) * 8, 8), 0:8].reshape(64, 128)[:, 64:128]
    flip = link_lanes(links, jnp.where(is_first, 0, 1), 2)
    row = moved(parts(jnp.where(flip != 1.0, mine, 0.0)), identity(64), (0, 0)) + moved(
        parts(jnp.where(flip == 1.0, mirrored, 0.0)), reversal(64), (0, 0)
    )
    row = joined(row[0:32], row[32:64]) + local[...]
    west = arrived[lax.rem(tile_row + nt - 1, nt), 8:40] + jnp.where(is_first, row, 0.0)
    east = arrived[lax.rem(tile_row + 1, nt), 8:40] + jnp.where(is_last, row, 0.0)
    return west, east, spread_out(south), spread_out(north)


def image_kernel(
    nt,
    nq,
    links,
    arrived,
    local,
    halos,
    fields,
    probes,
    spread,
    wind,
    misfit,
    costs,
    strips,
    top,
    bottom,
):
    west, east, south, north = outer_values(nt, nq, links, arrived, local, halos)
    planes = {}
    for pp in range(3):
        u = pair(wind, (0, 0), pp)
        v = pair(wind, (1, 0), pp)
        for probe in range(PROBES):
            field = lambda n: fields[(FORWARD.index(n) * PROBES + probe) * 3 + pp]
            at = lambda n, t: (list(t).index(n) * PROBES + probe) * 3 + pp
            dx = {n: slopes_x(field(n), at(n, FORWARD_X), west, east) for n in FORWARD_X}
            dy = {n: slopes_y(field(n), at(n, FORWARD_Y), south, north) for n in FORWARD_Y}
            thickness = pair(spread, (2, 0), pp) * pair(probes, (probe, 2, 0), pp)
            z = field("zonal") - dt * (dx["geo"] + u * dx["zonal"] + v * dy["zonal"])
            m = field("meridional") - dt * (
                dy["geo"] + u * dx["meridional"] + v * dy["meridional"]
            )
            t = thickness - dt * (dx["flux_x"] + dy["flux_y"])
            h = field("temp") - dt * (u * dx["temp"] + v * dy["temp"])
            z, m, t, h = (pair(misfit, (c, 0), pp) * w for c, w in enumerate((z, m, t, h)))
            for c, w in enumerate((z, m, t, h)):
                costs[(c * PROBES + probe) * 3 + pp] = w
            made = (u * z, u * m, v * z, v * m, z, m, t, u * h, v * h)
            for n, w in zip(ADJOINT, made):
                planes[n, probe, pp] = w
    put_strips(
        [planes[n, pr, pp] for n in ADJOINT for pr in range(PROBES) for pp in range(3)],
        strips,
        lax.axis_index("tx"),
    )
    put_outer_rows(
        [planes[n, pr, pp] for n in ADJOINT_X for pr in range(PROBES) for pp in range(3)],
        top,
        bottom,
    )


def adjoint_kernel(
    nt,
    nq,
    levels,
    links,
    arrived,
    local,
    halos,
    costs,
    wind,
    mass,
    heat,
    backs,
    loads,
):
    west, east, south, north = outer_values(nt, nq, links, arrived, local, halos)
    for pp in range(3):
        u = pair(wind, (0, 0), pp)
        v = pair(wind, (1, 0), pp)
        mass_here = pair(mass, (0,), pp)
        heat_here = pair(heat, (0,), pp)
        for probe in range(PROBES):
            z, m, t, h = (costs[(c * PROBES + probe) * 3 + pp] for c in range(4))
            field = dict(
                zip(ADJOINT, (u * z, u * m, v * z, v * m, z, m, t, u * h, v * h))
            )
            at = lambda n, k: (list(k).index(n) * PROBES + probe) * 3 + pp
            dx = {n: slopes_x(field[n], at(n, ADJOINT_X), west, east) for n in ADJOINT_X}
            dy = {n: slopes_y(field[n], at(n, ADJOINT_Y), south, north) for n in ADJOINT_Y}
            geo_back = dt * (dx["z"] + dy["m"])
            flux_x_back = dt * dx["t"]
            flux_y_back = dt * dy["t"]
            out = (
                z + dt * (dx["ez"] + dy["nz"]) + mass_here * flux_x_back,
                m + dt * (dx["em"] + dy["nm"]) + mass_here * flux_y_back,
                t + u * flux_x_back + v * flux_y_back,
                h + dt * (dx["eh"] + dy["nh"]) + geo_back,
            )
            for c, w in enumerate(out):
                backs[(c * PROBES + probe) * 3 + pp] = w
            load = heat_here * geo_back
            for k in range(levels):
                loads[k, (probe * 3 + pp) * 8 : (probe * 3 + pp) * 8 + 8] = load


def final_kernel(level_count, probes, spread, backs, loads, out):
    level = lax.axis_index("face")
    for probe in range(PROBES):
        for pp in range(3):
            at = (probe * 3 + pp) * 8
            load = jnp.zeros((8, 128), jnp.float32)
            for k in range(level_count):
                load = load + jnp.where(k >= level, loads[k, at : at + 8], 0.0)
            for c in range(4):
                back = backs[(c * PROBES + probe) * 3 + pp]
                if c == 2:
                    back = back + load
                for side in range(2):
                    part = back[:, 64 * side : 64 * side + 64]
                    p = 2 * pp + side
                    out[probe, c, 0, p] = probes[probe, c, 0, p] + spread[c, 0, p] * part


SMEM = pl.BlockSpec(memory_space=pltpu.SMEM)
VMEM = pl.BlockSpec(memory_space=pltpu.VMEM)
INTERPRET = False
GRANT = 8 << 20


def call(kernel, name, small, operands, shapes):
    shapes = [jax.ShapeDtypeStruct(s, jnp.float32) for s in shapes]
    return pl.pallas_call(
        kernel,
        name=name,
        out_shape=shapes,
        in_specs=[SMEM] * len(small) + [VMEM] * len(operands),
        out_specs=[VMEM] * len(shapes),
        compiler_params=pltpu.CompilerParams(vmem_limit_bytes=GRANT),
        interpret=INTERPRET,
    )(*small, *operands)


def thickness_copies(slots, probes, spread):
    return pl.pallas_call(
        functools.partial(thickness_kernel, slots),
        name="thickness",
        grid=(1,),
        out_shape=jax.ShapeDtypeStruct((slots, 48, 128), jnp.float32),
        in_specs=[
            pl.BlockSpec((PROBES, 1, 1, 6, 8, 64), lambda i: (0, 2, 0, 0, 0, 0)),
            pl.BlockSpec((1, 1, 6, 8, 64), lambda i: (2, 0, 0, 0, 0)),
        ],
        out_specs=pl.BlockSpec((slots, 48, 128), lambda i: (0, 0, 0)),
        interpret=INTERPRET,
    )(probes, spread)


def exchange(kind, nt, nq, links, strips, top, bottom):
    sources, x_targets, y_targets = TABLES[kind]
    codes = jnp.asarray(codes_of(sources, x_targets, y_targets))
    picks = jnp.asarray(picks_of(sources, y_targets))
    gathered = lax.all_gather(strips, "ty", axis=0)
    slots, local, halos = call(
        functools.partial(route_kernel, nt, nq),
        "route_" + kind,
        (links,),
        (gathered, top, bottom, codes, picks),
        ((nt, 40, 128), (32, 128), (16, 64)),
    )
    arrived = lax.all_to_all(slots, "tx", 0, 0, tiled=True)
    return arrived, local, halos


def body(probes, wind, mass, heat, spread, misfit, links):
    nf, nt, nq = (lax.axis_size(a) for a in ("face", "tx", "ty"))
    sent = thickness_copies(nf, probes, spread)
    totals = lax.all_to_all(sent, "face", 0, 0, tiled=True)
    fields, strips, top, bottom = call(
        functools.partial(fields_kernel, nf),
        "fields",
        (),
        (probes, spread, wind, mass, heat, totals),
        ((36, 8, 128), (STRIP, 128), (32, 128), (32, 128)),
    )
    outer = exchange("forward", nt, nq, links, strips, top, bottom)
    costs, strips, top, bottom = call(
        functools.partial(image_kernel, nt, nq),
        "image",
        (links,),
        (*outer, fields, probes, spread, wind, misfit),
        ((24, 8, 128), (STRIP, 128), (32, 128), (32, 128)),
    )
    outer = exchange("adjoint", nt, nq, links, strips, top, bottom)
    backs, loads = call(
        functools.partial(adjoint_kernel, nt, nq, nf),
        "adjoint",
        (links,),
        (*outer, costs, wind, mass, heat),
        ((24, 8, 128), (nf, 48, 128)),
    )
    loads = lax.all_to_all(loads, "face", 0, 0, tiled=True)
    (applied,) = call(
        functools.partial(final_kernel, nf),
        "final",
        (),
        (probes, spread, backs, loads),
        (probes.shape,),
    )
    return applied


def solution(mesh):
    return jax.shard_map(
        body,
        mesh=mesh,
        in_specs=(
            P(None, None, "face", None, "tx", "ty"),
            P(None, "face", None, "tx", "ty"),
            P("face", None, "tx", "ty"),
            P("face", None, "tx", "ty"),
            P(None, "face", None, "tx", "ty"),
            P(None, "face", None, "tx", "ty"),
            P(),
        ),
        out_specs=P(None, None, "face", None, "tx", "ty"),
        check_vma=False,
    )
```

```python
import functools

import jax
import jax.numpy as jnp
import numpy as np
from jax import lax
from jax.experimental import pallas as pl
from jax.experimental.pallas import tpu as pltpu
from jax.sharding import PartitionSpec as P

dt = 0.3
PROBES = 2
FORWARD = ("zonal", "meridional", "flux_x", "flux_y", "temp", "geo")
FORWARD_X = {
    "geo": {"geo": (0, 0)},
    "zonal": {"zonal": (1, 0), "meridional": (2, 0)},
    "meridional": {"zonal": (3, 0), "meridional": (4, 0)},
    "flux_x": {"flux_x": (1, 0), "flux_y": (2, 0)},
    "temp": {"temp": (0, 0)},
}
FORWARD_Y = {
    "geo": {"geo": (0, 0)},
    "zonal": {"zonal": (1, 0), "meridional": (2, 0)},
    "meridional": {"zonal": (3, 0), "meridional": (4, 0)},
    "flux_y": {"flux_x": (3, 0), "flux_y": (4, 0)},
    "temp": {"temp": (0, 0)},
}
ADJOINT = ("ez", "em", "nz", "nm", "z", "m", "t", "eh", "nh")
ADJOINT_X = {
    "ez": {"ez": (1, 1), "em": (1, 2), "nz": (2, 1), "nm": (2, 2)},
    "em": {"ez": (1, 3), "em": (1, 4), "nz": (2, 3), "nm": (2, 4)},
    "z": {"z": (1, 0), "m": (2, 0)},
    "t": {"t": (0, 0)},
    "eh": {"eh": (1, 0), "nh": (2, 0)},
}
ADJOINT_Y = {
    "nz": {"ez": (3, 1), "em": (3, 2), "nz": (4, 1), "nm": (4, 2)},
    "nm": {"ez": (3, 3), "em": (3, 4), "nz": (4, 3), "nm": (4, 4)},
    "m": {"z": (3, 0), "m": (4, 0)},
    "t": {"t": (0, 0)},
    "nh": {"eh": (3, 0), "nh": (4, 0)},
}
ROWS = 56
STRIP = 16 + ROWS


def source_index(unit, panel):
    return (panel % 2) * 64 + unit * 3 + panel // 2


def target_index(unit, panel):
    return (panel % 2) * 32 + unit * 3 + panel // 2


def codes_of(sources, x_targets, y_targets):
    codes = np.full((5, 128, 64), -1.0, np.float32)
    for d, targets in enumerate((x_targets, y_targets)):
        for t, (_, terms) in enumerate(targets.items()):
            for name, (i, j) in terms.items():
                s = sources.index(name)
                for probe in range(PROBES):
                    for n in range(6):
                        for f in range(6):
                            r = source_index(s * PROBES + probe, n)
                            c = target_index(t * PROBES + probe, f)
                            codes[2 * d, r, c] = i
                            codes[2 * d + 1, r, c] = j
    for u in range(len(sources) * PROBES):
        for n in range(6):
            codes[4, source_index(u, n), :] = n
    return codes


def picks_of(sources, y_targets):
    picks = np.zeros((128, 64), np.float32)
    for t, name in enumerate(y_targets):
        for probe in range(PROBES):
            for f in range(6):
                picks[
                    source_index(sources.index(name) * PROBES + probe, f),
                    target_index(t * PROBES + probe, f),
                ] = 1.0
    return picks


TABLES = {
    "forward": (FORWARD, FORWARD_X, FORWARD_Y),
    "adjoint": (ADJOINT, ADJOINT_X, ADJOINT_Y),
}


def parts(data):
    high = data.astype(jnp.bfloat16)
    rest = data - high.astype(jnp.float32)
    middle = rest.astype(jnp.bfloat16)
    low = (rest - middle.astype(jnp.float32)).astype(jnp.bfloat16)
    return high, middle, low


def product(a, b, contract):
    return lax.dot_general(
        a,
        b,
        (((contract[0],), (contract[1],)), ((), ())),
        preferred_element_type=jnp.float32,
    )


def moved(data, choice, contract=(1, 0)):
    high, middle, low = (product(d, choice, contract) for d in data)
    return (high + middle) + low


def chosen(choice, data, contract=(1, 0)):
    high, middle, low = (product(choice, d, contract) for d in data)
    return (high + middle) + low


def reversal(size):
    row = lax.broadcasted_iota(jnp.int32, (size, size), 0)
    column = lax.broadcasted_iota(jnp.int32, (size, size), 1)
    return (row + column == size - 1).astype(jnp.float32).astype(jnp.bfloat16)


def identity(size):
    row = lax.broadcasted_iota(jnp.int32, (size, size), 0)
    column = lax.broadcasted_iota(jnp.int32, (size, size), 1)
    return (row == column).astype(jnp.float32).astype(jnp.bfloat16)


def lanes(shape):
    return lax.broadcasted_iota(jnp.int32, shape, len(shape) - 1)


def joined(even, odd):
    return jnp.concatenate([even, odd], axis=1)


def joined_all(pieces):
    return jnp.concatenate(pieces, axis=1)


def pair(ref, index, pp):
    return joined(ref[(*index, 2 * pp)], ref[(*index, 2 * pp + 1)])


def link_lanes(links, edge, item):
    lane = lanes((1, 64))
    within = jnp.where(lane >= 32, lane - 32, lane)
    third = within - 3 * ((within * 43) // 128)
    out = jnp.zeros((1, 64), jnp.float32)
    for f in range(6):
        value = links[f, edge, item].astype(jnp.float32)
        here = (third == f // 2) & ((lane >= 32) == (f % 2 == 1))
        out = jnp.where(here, value, out)
    return out


def coefficients(links, edge, code_a, code_b, panel):
    one = jnp.ones((1, 64), jnp.float32)
    entries = [one] + [link_lanes(links, edge, 3 + k) for k in range(4)]
    a = jnp.zeros(code_a.shape, jnp.float32)
    b = jnp.zeros(code_a.shape, jnp.float32)
    for k in range(5):
        a = jnp.where(code_a == k, entries[k], a)
        b = jnp.where(code_b == k, entries[k], b)
    return jnp.where(panel == link_lanes(links, edge, 0), a * b, 0.0)


def put_strips(planes, out_ref, tile_row):
    lane = lanes((8, 128))
    south = jnp.zeros((8, 128), jnp.float32)
    north = jnp.zeros((8, 128), jnp.float32)
    rows = []
    for a, plane in enumerate(planes):
        here = (lane == a) | (lane == a + 64)
        south = jnp.where(here, plane if a == 0 else pltpu.roll(plane, a, 1), south)
        shift = (a - 63) % 128
        north = jnp.where(here, plane if shift == 0 else pltpu.roll(plane, shift, 1), north)
        rows.append(jnp.where(tile_row == 0, plane[0:1], plane[7:8]))
    out_ref[0:8] = south
    out_ref[8:16] = north
    rows.append(jnp.zeros((ROWS - len(rows), 128), jnp.float32))
    out_ref[16:STRIP] = jnp.concatenate(rows, axis=0)


def put_outer_rows(planes, top_ref, bottom_ref):
    spare = [jnp.zeros((32 - len(planes), 128), jnp.float32)]
    top_ref[...] = jnp.concatenate([p[0:1] for p in planes] + spare, axis=0)
    bottom_ref[...] = jnp.concatenate([p[7:8] for p in planes] + spare, axis=0)


def slopes_x(plane, b, west, east):
    row = lax.broadcasted_iota(jnp.int32, (8, 128), 0)
    after = jnp.where(row == 7, east[b : b + 1], pltpu.roll(plane, 7, 0))
    before = jnp.where(row == 0, west[b : b + 1], pltpu.roll(plane, 1, 0))
    return 0.5 * (after - before)


def slopes_y(plane, b, south, north):
    lane = lanes((8, 128))
    low = (lane == 0) | (lane == 64)
    high = (lane == 63) | (lane == 127)
    from_south = south if b == 0 else pltpu.roll(south, 128 - b, 1)
    after = jnp.where(high, pltpu.roll(north, 63 - b, 1), pltpu.roll(plane, 127, 1))
    before = jnp.where(low, from_south, pltpu.roll(plane, 1, 1))
    return 0.5 * (after - before)


def thickness_kernel(slots, probes, spread, out):
    for probe in range(PROBES):
        for pp in range(3):
            value = pair(spread, (0, 0), pp) * pair(probes, (probe, 0, 0), pp)
            for k in range(slots):
                out[k, (probe * 3 + pp) * 8 : (probe * 3 + pp) * 8 + 8] = value


def fields_kernel(
    level_count, probes, spread, wind, mass, heat, totals, fields, strips, top, bottom
):
    level, tile_row = lax.axis_index("face"), lax.axis_index("tx")
    planes = {}
    for pp in range(3):
        east = pair(wind, (0, 0), pp)
        north = pair(wind, (1, 0), pp)
        mass_here = pair(mass, (0,), pp)
        heat_here = pair(heat, (0,), pp)
        for probe in range(PROBES):
            scaled = [
                pair(spread, (c, 0), pp) * pair(probes, (probe, c, 0), pp) for c in range(4)
            ]
            zonal, meridional, thickness, temp = scaled
            at = (probe * 3 + pp) * 8
            pressure = thickness
            for k in range(level_count - 1):
                pressure = pressure + jnp.where(k < level, totals[k, at : at + 8], 0.0)
            planes["zonal", probe, pp] = zonal
            planes["meridional", probe, pp] = meridional
            planes["flux_x", probe, pp] = east * thickness + mass_here * zonal
            planes["flux_y", probe, pp] = north * thickness + mass_here * meridional
            planes["temp", probe, pp] = temp
            planes["geo", probe, pp] = temp + heat_here * pressure
    ordered = [planes[n, pr, pp] for n in FORWARD for pr in range(PROBES) for pp in range(3)]
    for a, plane in enumerate(ordered):
        fields[a] = plane
    put_strips(ordered, strips, tile_row)
    put_outer_rows(
        [planes[n, pr, pp] for n in FORWARD_X for pr in range(PROBES) for pp in range(3)],
        top,
        bottom,
    )


def route_kernel(
    nt, nq, links, gathered, top, bottom, codes, picks, slots, swap_a, swap_b, local, halos
):
    tile_row, tile_column = lax.axis_index("tx"), lax.axis_index("ty")
    is_first, is_last = tile_row == 0, tile_row == nt - 1
    line_f = jnp.where(is_first, 0.0, 1.0)
    column_edge = jnp.where(tile_column == 0, 2, 3)
    panel = codes[4]
    c0 = coefficients(links, 0, codes[0], codes[1], panel)
    c1 = coefficients(links, 1, codes[0], codes[1], panel)
    cc = coefficients(links, column_edge, codes[2], codes[3], panel)
    ends = joined(c0, c1).astype(jnp.bfloat16)
    cc = cc.astype(jnp.bfloat16)

    def masks(edge, source):
        far = link_lanes(links, edge, 1)
        flip = link_lanes(links, edge, 2)
        here = far == source
        return (
            jnp.where(here & (flip != 1.0), 1.0, 0.0),
            jnp.where(here & (flip == 1.0), 1.0, 0.0),
        )

    back64 = reversal(64)
    empty = jnp.zeros((64 - ROWS, 64), jnp.float32)

    def segment(q):
        packed = gathered[q, 16:STRIP]
        return parts(
            jnp.concatenate([packed[:, 0:64], empty, packed[:, 64:128], empty], axis=0)
        )

    on_boundary = jnp.where(is_first | is_last, 1.0, 0.0)
    plain_c, turned_c = masks(column_edge, line_f)
    across = [moved(segment(q), cc, (0, 0)) * on_boundary for q in range(nq)]
    turned = joined_all([a * turned_c for a in across])
    turned = chosen(back64, parts(turned))
    pieces = [
        across[q] * plain_c + turned[:, 64 * (nq - 1 - q) : 64 * (nq - q)] for q in range(nq)
    ]
    columns = parts(jnp.concatenate([gathered[0, 0:8], gathered[nq - 1, 8:16]], axis=0))
    low_plain, low_turned = masks(column_edge, 2.0)
    high_plain, high_turned = masks(column_edge, 3.0)
    to_columns = moved(columns, cc)
    low_c, high_c = to_columns[0:8], to_columns[8:16]
    straight = low_c * low_plain + high_c * high_plain
    flipped = chosen(reversal(8), parts(low_c * low_turned + high_c * high_turned))
    to_rows = moved(columns, ends)
    far = joined(link_lanes(links, 0, 1), link_lanes(links, 1, 1))
    to_rows = to_rows[0:8] * jnp.where(far == 2.0, 1.0, 0.0) + to_rows[8:16] * jnp.where(
        far == 3.0, 1.0, 0.0
    )
    to_rows = [to_rows[:, 0:64], to_rows[:, 64:128]]
    for t in range(nt):
        q, at = t // 8, (t % 8) * 8
        left = pieces[q][at : at + 8]
        left = left + jnp.where(tile_row == t, straight, 0.0)
        left = left + jnp.where(tile_row == nt - 1 - t, flipped, 0.0)
        slots[t] = joined(left, to_rows[1] if t == nt - 1 else to_rows[0])

    plain0, turned0 = masks(0, line_f)
    plain1, turned1 = masks(1, line_f)
    plain = (joined(c0, c1) * joined(plain0, plain1)).astype(jnp.bfloat16)
    mirror = (joined(c0, c1) * joined(turned0, turned1)).astype(jnp.bfloat16)
    by_row = chosen(plain, segment(tile_column), (0, 0))
    by_row = by_row + moved(
        parts(chosen(mirror, segment(nq - 1 - tile_column), (0, 0))), back64
    )
    by_row = [joined(by_row[k : k + 32], by_row[k + 32 : k + 64]) for k in (0, 64)]
    local[...] = jnp.where(is_first, by_row[0], by_row[1])
    to_lower = jnp.where(is_first, by_row[1], top[...])
    to_upper = jnp.where(is_last, by_row[0], bottom[...])
    even = lax.rem(tile_row, 2) == 0
    swap_a[...] = jnp.where(even, to_upper, to_lower)
    swap_b[...] = jnp.where(even, to_lower, to_upper)

    below = gathered[jnp.maximum(tile_column - 1, 0), 8:16]
    above = gathered[jnp.minimum(tile_column + 1, nq - 1), 0:8]
    near = moved(parts(jnp.concatenate([below, above], axis=0)), picks[...].astype(jnp.bfloat16))
    halos[0:8] = jnp.where(tile_column > 0, near[0:8], 0.0)
    halos[8:16] = jnp.where(tile_column < nq - 1, near[8:16], 0.0)


def collect_kernel(nt, nq, links, arrived, local, halos, sides, row_out):
    tile_row, tile_column = lax.axis_index("tx"), lax.axis_index("ty")
    is_first, is_last = tile_row == 0, tile_row == nt - 1
    column = arrived[0]
    for t in range(1, nt):
        column = column + arrived[t]
    column = column[:, 0:64]
    lane = lanes((8, 128))

    def spread_out(narrow):
        wide = joined(narrow, narrow)
        return jnp.where(lane < 32, wide, pltpu.roll(wide, 32, 1))

    sides[0:8] = spread_out(halos[0:8] + jnp.where(tile_column == 0, column, 0.0))
    sides[8:16] = spread_out(halos[8:16] + jnp.where(tile_column == nq - 1, column, 0.0))
    mine = arrived[pl.ds(tile_column * 8, 8)].reshape(64, 128)[:, 64:128]
    mirrored = arrived[pl.ds((nq - 1 - tile_column) * 8, 8)].reshape(64, 128)[:, 64:128]
    flip = link_lanes(links, jnp.where(is_first, 0, 1), 2)
    row = moved(parts(jnp.where(flip != 1.0, mine, 0.0)), identity(64), (0, 0)) + moved(
        parts(jnp.where(flip == 1.0, mirrored, 0.0)), reversal(64), (0, 0)
    )
    row_out[...] = joined(row[0:32], row[32:64]) + local[...]


def outer_values(nt, sides, row, swapped_a, swapped_b):
    tile_row = lax.axis_index("tx")
    even = lax.rem(tile_row, 2) == 0
    west = jnp.where(even, swapped_b[...], swapped_a[...])
    east = jnp.where(even, swapped_a[...], swapped_b[...])
    west = west + jnp.where(tile_row == 0, row[...], 0.0)
    east = east + jnp.where(tile_row == nt - 1, row[...], 0.0)
    return west, east, sides[0:8], sides[8:16]


def image_kernel(
    nt,
    sides,
    row,
    swapped_a,
    swapped_b,
    fields,
    probes,
    spread,
    wind,
    misfit,
    costs,
    strips,
    top,
    bottom,
):
    west, east, south, north = outer_values(nt, sides, row, swapped_a, swapped_b)
    planes = {}
    for pp in range(3):
        u = pair(wind, (0, 0), pp)
        v = pair(wind, (1, 0), pp)
        for probe in range(PROBES):
            field = lambda n: fields[(FORWARD.index(n) * PROBES + probe) * 3 + pp]
            at = lambda n, t: (list(t).index(n) * PROBES + probe) * 3 + pp
            dx = {n: slopes_x(field(n), at(n, FORWARD_X), west, east) for n in FORWARD_X}
            dy = {n: slopes_y(field(n), at(n, FORWARD_Y), south, north) for n in FORWARD_Y}
            thickness = pair(spread, (2, 0), pp) * pair(probes, (probe, 2, 0), pp)
            z = field("zonal") - dt * (dx["geo"] + u * dx["zonal"] + v * dy["zonal"])
            m = field("meridional") - dt * (
                dy["geo"] + u * dx["meridional"] + v * dy["meridional"]
            )
            t = thickness - dt * (dx["flux_x"] + dy["flux_y"])
            h = field("temp") - dt * (u * dx["temp"] + v * dy["temp"])
            z, m, t, h = (pair(misfit, (c, 0), pp) * w for c, w in enumerate((z, m, t, h)))
            for c, w in enumerate((z, m, t, h)):
                costs[(c * PROBES + probe) * 3 + pp] = w
            made = (u * z, u * m, v * z, v * m, z, m, t, u * h, v * h)
            for n, w in zip(ADJOINT, made):
                planes[n, probe, pp] = w
    put_strips(
        [planes[n, pr, pp] for n in ADJOINT for pr in range(PROBES) for pp in range(3)],
        strips,
        lax.axis_index("tx"),
    )
    put_outer_rows(
        [planes[n, pr, pp] for n in ADJOINT_X for pr in range(PROBES) for pp in range(3)],
        top,
        bottom,
    )


def adjoint_kernel(
    nt,
    levels,
    sides,
    row,
    swapped_a,
    swapped_b,
    costs,
    wind,
    mass,
    heat,
    backs,
    loads,
):
    west, east, south, north = outer_values(nt, sides, row, swapped_a, swapped_b)
    for pp in range(3):
        u = pair(wind, (0, 0), pp)
        v = pair(wind, (1, 0), pp)
        mass_here = pair(mass, (0,), pp)
        heat_here = pair(heat, (0,), pp)
        for probe in range(PROBES):
            z, m, t, h = (costs[(c * PROBES + probe) * 3 + pp] for c in range(4))
            field = dict(
                zip(ADJOINT, (u * z, u * m, v * z, v * m, z, m, t, u * h, v * h))
            )
            at = lambda n, k: (list(k).index(n) * PROBES + probe) * 3 + pp
            dx = {n: slopes_x(field[n], at(n, ADJOINT_X), west, east) for n in ADJOINT_X}
            dy = {n: slopes_y(field[n], at(n, ADJOINT_Y), south, north) for n in ADJOINT_Y}
            geo_back = dt * (dx["z"] + dy["m"])
            flux_x_back = dt * dx["t"]
            flux_y_back = dt * dy["t"]
            out = (
                z + dt * (dx["ez"] + dy["nz"]) + mass_here * flux_x_back,
                m + dt * (dx["em"] + dy["nm"]) + mass_here * flux_y_back,
                t + u * flux_x_back + v * flux_y_back,
                h + dt * (dx["eh"] + dy["nh"]) + geo_back,
            )
            for c, w in enumerate(out):
                backs[(c * PROBES + probe) * 3 + pp] = w
            load = heat_here * geo_back
            for k in range(levels):
                loads[k, (probe * 3 + pp) * 8 : (probe * 3 + pp) * 8 + 8] = load


def final_kernel(level_count, probes, spread, backs, loads, out):
    level = lax.axis_index("face")
    for probe in range(PROBES):
        for pp in range(3):
            at = (probe * 3 + pp) * 8
            load = jnp.zeros((8, 128), jnp.float32)
            for k in range(level_count):
                load = load + jnp.where(k >= level, loads[k, at : at + 8], 0.0)
            for c in range(4):
                back = backs[(c * PROBES + probe) * 3 + pp]
                if c == 2:
                    back = back + load
                for side in range(2):
                    part = back[:, 64 * side : 64 * side + 64]
                    p = 2 * pp + side
                    out[probe, c, 0, p] = probes[probe, c, 0, p] + spread[c, 0, p] * part


SMEM = pl.BlockSpec(memory_space=pltpu.SMEM)
VMEM = pl.BlockSpec(memory_space=pltpu.VMEM)
INTERPRET = False
GRANT = 8 << 20


def call(kernel, small, operands, shapes):
    shapes = [jax.ShapeDtypeStruct(s, jnp.float32) for s in shapes]
    return pl.pallas_call(
        kernel,
        out_shape=shapes,
        in_specs=[SMEM] * len(small) + [VMEM] * len(operands),
        out_specs=[VMEM] * len(shapes),
        compiler_params=pltpu.CompilerParams(vmem_limit_bytes=GRANT),
        interpret=INTERPRET,
    )(*small, *operands)


def thickness_copies(slots, probes, spread):
    return pl.pallas_call(
        functools.partial(thickness_kernel, slots),
        name="thickness",
        grid=(1,),
        out_shape=jax.ShapeDtypeStruct((slots, 48, 128), jnp.float32),
        in_specs=[
            pl.BlockSpec((PROBES, 1, 1, 6, 8, 64), lambda i: (0, 2, 0, 0, 0, 0)),
            pl.BlockSpec((1, 1, 6, 8, 64), lambda i: (2, 0, 0, 0, 0)),
        ],
        out_specs=pl.BlockSpec((slots, 48, 128), lambda i: (0, 0, 0)),
        interpret=INTERPRET,
    )(probes, spread)


def exchange(kind, nt, nq, links, strips, top, bottom):
    sources, x_targets, y_targets = TABLES[kind]
    codes = jnp.asarray(codes_of(sources, x_targets, y_targets))
    picks = jnp.asarray(picks_of(sources, y_targets))
    gathered = lax.all_gather(strips, "ty", axis=0)
    slots, swap_a, swap_b, local, halos = call(
        functools.partial(route_kernel, nt, nq),
        (links,),
        (gathered, top, bottom, codes, picks),
        ((nt, 8, 128), (32, 128), (32, 128), (32, 128), (16, 64)),
    )
    near = [(i, i ^ 1) for i in range(nt)]
    wrapped = [(i, (i + 1 if i % 2 else i - 1) % nt) for i in range(nt)]
    swapped_a = lax.ppermute(swap_a, "tx", near)
    swapped_b = lax.ppermute(swap_b, "tx", wrapped)
    arrived = lax.all_to_all(slots, "tx", 0, 0, tiled=True)
    sides, row = call(
        functools.partial(collect_kernel, nt, nq),
        (links,),
        (arrived, local, halos),
        ((16, 128), (32, 128)),
    )
    return sides, row, swapped_a, swapped_b


def body(probes, wind, mass, heat, spread, misfit, links):
    nf, nt, nq = (lax.axis_size(a) for a in ("face", "tx", "ty"))
    sent = thickness_copies(nf, probes, spread)
    totals = lax.all_to_all(sent, "face", 0, 0, tiled=True)
    fields, strips, top, bottom = call(
        functools.partial(fields_kernel, nf),
        (),
        (probes, spread, wind, mass, heat, totals),
        ((36, 8, 128), (STRIP, 128), (32, 128), (32, 128)),
    )
    outer = exchange("forward", nt, nq, links, strips, top, bottom)
    costs, strips, top, bottom = call(
        functools.partial(image_kernel, nt),
        (),
        (*outer, fields, probes, spread, wind, misfit),
        ((24, 8, 128), (STRIP, 128), (32, 128), (32, 128)),
    )
    outer = exchange("adjoint", nt, nq, links, strips, top, bottom)
    backs, loads = call(
        functools.partial(adjoint_kernel, nt, nf),
        (),
        (*outer, costs, wind, mass, heat),
        ((24, 8, 128), (nf, 48, 128)),
    )
    loads = lax.all_to_all(loads, "face", 0, 0, tiled=True)
    (applied,) = call(
        functools.partial(final_kernel, nf), (), (probes, spread, backs, loads), (probes.shape,)
    )
    return applied


def solution(mesh):
    return jax.shard_map(
        body,
        mesh=mesh,
        in_specs=(
            P(None, None, "face", None, "tx", "ty"),
            P(None, "face", None, "tx", "ty"),
            P("face", None, "tx", "ty"),
            P("face", None, "tx", "ty"),
            P(None, "face", None, "tx", "ty"),
            P(None, "face", None, "tx", "ty"),
            P(),
        ),
        out_specs=P(None, None, "face", None, "tx", "ty"),
        check_vma=False,
    )
```

```python
import functools

import jax
import jax.numpy as jnp
import numpy as np
from jax import lax
from jax.experimental import pallas as pl
from jax.experimental.pallas import tpu as pltpu
from jax.sharding import PartitionSpec as P

dt = 0.3
PROBES = 2
FORWARD = ("zonal", "meridional", "flux_x", "flux_y", "temp", "geo")
FORWARD_X = {
    "geo": {"geo": (0, 0)},
    "zonal": {"zonal": (1, 0), "meridional": (2, 0)},
    "meridional": {"zonal": (3, 0), "meridional": (4, 0)},
    "flux_x": {"flux_x": (1, 0), "flux_y": (2, 0)},
    "temp": {"temp": (0, 0)},
}
FORWARD_Y = {
    "geo": {"geo": (0, 0)},
    "zonal": {"zonal": (1, 0), "meridional": (2, 0)},
    "meridional": {"zonal": (3, 0), "meridional": (4, 0)},
    "flux_y": {"flux_x": (3, 0), "flux_y": (4, 0)},
    "temp": {"temp": (0, 0)},
}
ADJOINT = ("ez", "em", "nz", "nm", "z", "m", "t", "eh", "nh")
ADJOINT_X = {
    "ez": {"ez": (1, 1), "em": (1, 2), "nz": (2, 1), "nm": (2, 2)},
    "em": {"ez": (1, 3), "em": (1, 4), "nz": (2, 3), "nm": (2, 4)},
    "z": {"z": (1, 0), "m": (2, 0)},
    "t": {"t": (0, 0)},
    "eh": {"eh": (1, 0), "nh": (2, 0)},
}
ADJOINT_Y = {
    "nz": {"ez": (3, 1), "em": (3, 2), "nz": (4, 1), "nm": (4, 2)},
    "nm": {"ez": (3, 3), "em": (3, 4), "nz": (4, 3), "nm": (4, 4)},
    "m": {"z": (3, 0), "m": (4, 0)},
    "t": {"t": (0, 0)},
    "nh": {"eh": (3, 0), "nh": (4, 0)},
}
ROWS = 56
STRIP = 16 + ROWS


def source_index(unit, panel):
    return (panel % 2) * 64 + unit * 3 + panel // 2


def target_index(unit, panel):
    return (panel % 2) * 32 + unit * 3 + panel // 2


def codes_of(sources, x_targets, y_targets):
    codes = np.full((5, 128, 64), -1.0, np.float32)
    for d, targets in enumerate((x_targets, y_targets)):
        for t, (_, terms) in enumerate(targets.items()):
            for name, (i, j) in terms.items():
                s = sources.index(name)
                for probe in range(PROBES):
                    for n in range(6):
                        for f in range(6):
                            r = source_index(s * PROBES + probe, n)
                            c = target_index(t * PROBES + probe, f)
                            codes[2 * d, r, c] = i
                            codes[2 * d + 1, r, c] = j
    for u in range(len(sources) * PROBES):
        for n in range(6):
            codes[4, source_index(u, n), :] = n
    return codes


def picks_of(sources, y_targets):
    picks = np.zeros((128, 64), np.float32)
    for t, name in enumerate(y_targets):
        for probe in range(PROBES):
            for f in range(6):
                picks[
                    source_index(sources.index(name) * PROBES + probe, f),
                    target_index(t * PROBES + probe, f),
                ] = 1.0
    return picks


TABLES = {
    "forward": (FORWARD, FORWARD_X, FORWARD_Y),
    "adjoint": (ADJOINT, ADJOINT_X, ADJOINT_Y),
}


def parts(data):
    high = data.astype(jnp.bfloat16)
    rest = data - high.astype(jnp.float32)
    middle = rest.astype(jnp.bfloat16)
    low = (rest - middle.astype(jnp.float32)).astype(jnp.bfloat16)
    return high, middle, low


def product(a, b, contract):
    return lax.dot_general(
        a,
        b,
        (((contract[0],), (contract[1],)), ((), ())),
        preferred_element_type=jnp.float32,
    )


def moved(data, choice, contract=(1, 0)):
    high, middle, low = (product(d, choice, contract) for d in data)
    return (high + middle) + low


def chosen(choice, data, contract=(1, 0)):
    high, middle, low = (product(choice, d, contract) for d in data)
    return (high + middle) + low


def reversal(size):
    row = lax.broadcasted_iota(jnp.int32, (size, size), 0)
    column = lax.broadcasted_iota(jnp.int32, (size, size), 1)
    return (row + column == size - 1).astype(jnp.float32).astype(jnp.bfloat16)


def identity(size):
    row = lax.broadcasted_iota(jnp.int32, (size, size), 0)
    column = lax.broadcasted_iota(jnp.int32, (size, size), 1)
    return (row == column).astype(jnp.float32).astype(jnp.bfloat16)


def lanes(shape):
    return lax.broadcasted_iota(jnp.int32, shape, len(shape) - 1)


def joined(even, odd):
    return jnp.concatenate([even, odd], axis=1)


def joined_all(pieces):
    return jnp.concatenate(pieces, axis=1)


def pair(ref, index, pp):
    return joined(ref[(*index, 2 * pp)], ref[(*index, 2 * pp + 1)])


def put_table(links, table):
    lane = lanes((1, 64))
    within = jnp.where(lane >= 32, lane - 32, lane)
    third = within - 3 * ((within * 43) // 128)
    here = [(third == f // 2) & ((lane >= 32) == (f % 2 == 1)) for f in range(6)]
    for edge in range(4):
        for item in range(7):
            out = jnp.zeros((1, 64), jnp.float32)
            for f in range(6):
                out = jnp.where(here[f], links[f, edge, item].astype(jnp.float32), out)
            table[edge, item : item + 1] = out
        table[edge, 7:8] = jnp.zeros((1, 64), jnp.float32)


def link_lanes(table, edge, item):
    return table[edge, item : item + 1]


def coefficients(links, edge, code_a, code_b, panel):
    one = jnp.ones((1, 64), jnp.float32)
    entries = [one] + [link_lanes(links, edge, 3 + k) for k in range(4)]
    a = jnp.zeros(code_a.shape, jnp.float32)
    b = jnp.zeros(code_a.shape, jnp.float32)
    for k in range(5):
        a = jnp.where(code_a == k, entries[k], a)
        b = jnp.where(code_b == k, entries[k], b)
    return jnp.where(panel == link_lanes(links, edge, 0), a * b, 0.0)


def put_strips(planes, out_ref, tile_row):
    lane = lanes((8, 128))
    south = jnp.zeros((8, 128), jnp.float32)
    north = jnp.zeros((8, 128), jnp.float32)
    rows = []
    for a, plane in enumerate(planes):
        here = (lane == a) | (lane == a + 64)
        south = jnp.where(here, plane if a == 0 else pltpu.roll(plane, a, 1), south)
        shift = (a - 63) % 128
        north = jnp.where(here, plane if shift == 0 else pltpu.roll(plane, shift, 1), north)
        rows.append(jnp.where(tile_row == 0, plane[0:1], plane[7:8]))
    out_ref[0:8] = south
    out_ref[8:16] = north
    rows.append(jnp.zeros((ROWS - len(rows), 128), jnp.float32))
    out_ref[16:STRIP] = jnp.concatenate(rows, axis=0)


def put_outer_rows(planes, near_ref, far_ref):
    spare = [jnp.zeros((32 - len(planes), 128), jnp.float32)]
    top = jnp.concatenate([p[0:1] for p in planes] + spare, axis=0)
    bottom = jnp.concatenate([p[7:8] for p in planes] + spare, axis=0)
    even = lax.rem(lax.axis_index("tx"), 2) == 0
    near_ref[...] = jnp.where(even, bottom, top)
    far_ref[...] = jnp.where(even, top, bottom)


def slopes_x(plane, b, west, east):
    row = lax.broadcasted_iota(jnp.int32, (8, 128), 0)
    after = jnp.where(row == 7, east[b : b + 1], pltpu.roll(plane, 7, 0))
    before = jnp.where(row == 0, west[b : b + 1], pltpu.roll(plane, 1, 0))
    return 0.5 * (after - before)


def slopes_y(plane, b, south, north):
    lane = lanes((8, 128))
    low = (lane == 0) | (lane == 64)
    high = (lane == 63) | (lane == 127)
    from_south = south if b == 0 else pltpu.roll(south, 128 - b, 1)
    after = jnp.where(high, pltpu.roll(north, 63 - b, 1), pltpu.roll(plane, 127, 1))
    before = jnp.where(low, from_south, pltpu.roll(plane, 1, 1))
    return 0.5 * (after - before)


def thickness_kernel(slots, links, probes, spread, out, table):
    put_table(links, table)
    for probe in range(PROBES):
        for pp in range(3):
            value = pair(spread, (0, 0), pp) * pair(probes, (probe, 0, 0), pp)
            for k in range(slots):
                out[k, (probe * 3 + pp) * 8 : (probe * 3 + pp) * 8 + 8] = value


def fields_kernel(
    level_count, probes, spread, wind, mass, heat, totals, fields, strips, near_row, far_row
):
    level, tile_row = lax.axis_index("face"), lax.axis_index("tx")
    planes = {}
    for pp in range(3):
        east = pair(wind, (0, 0), pp)
        north = pair(wind, (1, 0), pp)
        mass_here = pair(mass, (0,), pp)
        heat_here = pair(heat, (0,), pp)
        for probe in range(PROBES):
            scaled = [
                pair(spread, (c, 0), pp) * pair(probes, (probe, c, 0), pp) for c in range(4)
            ]
            zonal, meridional, thickness, temp = scaled
            at = (probe * 3 + pp) * 8
            pressure = thickness
            for k in range(level_count - 1):
                pressure = pressure + jnp.where(k < level, totals[k, at : at + 8], 0.0)
            planes["zonal", probe, pp] = zonal
            planes["meridional", probe, pp] = meridional
            planes["flux_x", probe, pp] = east * thickness + mass_here * zonal
            planes["flux_y", probe, pp] = north * thickness + mass_here * meridional
            planes["temp", probe, pp] = temp
            planes["geo", probe, pp] = temp + heat_here * pressure
    ordered = [planes[n, pr, pp] for n in FORWARD for pr in range(PROBES) for pp in range(3)]
    for a, plane in enumerate(ordered):
        fields[a] = plane
    put_strips(ordered, strips, tile_row)
    put_outer_rows(
        [planes[n, pr, pp] for n in FORWARD_X for pr in range(PROBES) for pp in range(3)],
        near_row,
        far_row,
    )


def route_kernel(
    nt, nq, links, gathered, far_row, codes, picks, slots, swap_b, local, halos
):
    tile_row, tile_column = lax.axis_index("tx"), lax.axis_index("ty")
    is_first, is_last = tile_row == 0, tile_row == nt - 1
    line_f = jnp.where(is_first, 0.0, 1.0)
    column_edge = jnp.where(tile_column == 0, 2, 3)
    panel = codes[4]
    c0 = coefficients(links, 0, codes[0], codes[1], panel)
    c1 = coefficients(links, 1, codes[0], codes[1], panel)
    cc = coefficients(links, column_edge, codes[2], codes[3], panel)
    ends = joined(c0, c1).astype(jnp.bfloat16)
    cc = cc.astype(jnp.bfloat16)

    def masks(edge, source):
        far = link_lanes(links, edge, 1)
        flip = link_lanes(links, edge, 2)
        here = far == source
        return (
            jnp.where(here & (flip != 1.0), 1.0, 0.0),
            jnp.where(here & (flip == 1.0), 1.0, 0.0),
        )

    back64 = reversal(64)
    empty = jnp.zeros((64 - ROWS, 64), jnp.float32)

    def segment(q):
        packed = gathered[q, 16:STRIP]
        return parts(
            jnp.concatenate([packed[:, 0:64], empty, packed[:, 64:128], empty], axis=0)
        )

    on_boundary = jnp.where(is_first | is_last, 1.0, 0.0)
    plain_c, turned_c = masks(column_edge, line_f)
    across = [moved(segment(q), cc, (0, 0)) * on_boundary for q in range(nq)]
    turned = joined_all([a * turned_c for a in across])
    turned = chosen(back64, parts(turned))
    pieces = [
        across[q] * plain_c + turned[:, 64 * (nq - 1 - q) : 64 * (nq - q)] for q in range(nq)
    ]
    columns = parts(jnp.concatenate([gathered[0, 0:8], gathered[nq - 1, 8:16]], axis=0))
    low_plain, low_turned = masks(column_edge, 2.0)
    high_plain, high_turned = masks(column_edge, 3.0)
    to_columns = moved(columns, cc)
    low_c, high_c = to_columns[0:8], to_columns[8:16]
    straight = low_c * low_plain + high_c * high_plain
    flipped = chosen(reversal(8), parts(low_c * low_turned + high_c * high_turned))
    to_rows = moved(columns, ends)
    far = joined(link_lanes(links, 0, 1), link_lanes(links, 1, 1))
    to_rows = to_rows[0:8] * jnp.where(far == 2.0, 1.0, 0.0) + to_rows[8:16] * jnp.where(
        far == 3.0, 1.0, 0.0
    )
    to_rows = [to_rows[:, 0:64], to_rows[:, 64:128]]
    for t in range(nt):
        q, at = t // 8, (t % 8) * 8
        left = pieces[q][at : at + 8]
        left = left + jnp.where(tile_row == t, straight, 0.0)
        left = left + jnp.where(tile_row == nt - 1 - t, flipped, 0.0)
        slots[t] = joined(left, to_rows[1] if t == nt - 1 else to_rows[0])

    plain0, turned0 = masks(0, line_f)
    plain1, turned1 = masks(1, line_f)
    plain = (joined(c0, c1) * joined(plain0, plain1)).astype(jnp.bfloat16)
    mirror = (joined(c0, c1) * joined(turned0, turned1)).astype(jnp.bfloat16)
    by_row = chosen(plain, segment(tile_column), (0, 0))
    by_row = by_row + moved(
        parts(chosen(mirror, segment(nq - 1 - tile_column), (0, 0))), back64
    )
    by_row = [joined(by_row[k : k + 32], by_row[k + 32 : k + 64]) for k in (0, 64)]
    local[...] = jnp.where(is_first, by_row[0], by_row[1])
    sent = jnp.where(is_first, by_row[1], far_row[...])
    swap_b[...] = jnp.where(is_last, by_row[0], sent)

    below = gathered[jnp.maximum(tile_column - 1, 0), 8:16]
    above = gathered[jnp.minimum(tile_column + 1, nq - 1), 0:8]
    near = moved(parts(jnp.concatenate([below, above], axis=0)), picks[...].astype(jnp.bfloat16))
    halos[0:8] = jnp.where(tile_column > 0, near[0:8], 0.0)
    halos[8:16] = jnp.where(tile_column < nq - 1, near[8:16], 0.0)


def collect_kernel(nt, nq, links, arrived, local, halos, sides, row_out):
    tile_row, tile_column = lax.axis_index("tx"), lax.axis_index("ty")
    is_first, is_last = tile_row == 0, tile_row == nt - 1
    column = arrived[0]
    for t in range(1, nt):
        column = column + arrived[t]
    column = column[:, 0:64]
    lane = lanes((8, 128))

    def spread_out(narrow):
        wide = joined(narrow, narrow)
        return jnp.where(lane < 32, wide, pltpu.roll(wide, 32, 1))

    sides[0:8] = spread_out(halos[0:8] + jnp.where(tile_column == 0, column, 0.0))
    sides[8:16] = spread_out(halos[8:16] + jnp.where(tile_column == nq - 1, column, 0.0))
    mine = arrived[pl.ds(tile_column * 8, 8)].reshape(64, 128)[:, 64:128]
    mirrored = arrived[pl.ds((nq - 1 - tile_column) * 8, 8)].reshape(64, 128)[:, 64:128]
    flip = link_lanes(links, jnp.where(is_first, 0, 1), 2)
    row = moved(parts(jnp.where(flip != 1.0, mine, 0.0)), identity(64), (0, 0)) + moved(
        parts(jnp.where(flip == 1.0, mirrored, 0.0)), reversal(64), (0, 0)
    )
    row_out[...] = joined(row[0:32], row[32:64]) + local[...]


def outer_values(nt, sides, row, swapped_a, swapped_b):
    tile_row = lax.axis_index("tx")
    even = lax.rem(tile_row, 2) == 0
    west = jnp.where(even, swapped_b[...], swapped_a[...])
    east = jnp.where(even, swapped_a[...], swapped_b[...])
    west = west + jnp.where(tile_row == 0, row[...], 0.0)
    east = east + jnp.where(tile_row == nt - 1, row[...], 0.0)
    return west, east, sides[0:8], sides[8:16]


def image_kernel(
    nt,
    sides,
    row,
    swapped_a,
    swapped_b,
    fields,
    probes,
    spread,
    wind,
    misfit,
    costs,
    strips,
    near_row,
    far_row,
):
    west, east, south, north = outer_values(nt, sides, row, swapped_a, swapped_b)
    planes = {}
    for pp in range(3):
        u = pair(wind, (0, 0), pp)
        v = pair(wind, (1, 0), pp)
        for probe in range(PROBES):
            field = lambda n: fields[(FORWARD.index(n) * PROBES + probe) * 3 + pp]
            at = lambda n, t: (list(t).index(n) * PROBES + probe) * 3 + pp
            dx = {n: slopes_x(field(n), at(n, FORWARD_X), west, east) for n in FORWARD_X}
            dy = {n: slopes_y(field(n), at(n, FORWARD_Y), south, north) for n in FORWARD_Y}
            thickness = pair(spread, (2, 0), pp) * pair(probes, (probe, 2, 0), pp)
            z = field("zonal") - dt * (dx["geo"] + u * dx["zonal"] + v * dy["zonal"])
            m = field("meridional") - dt * (
                dy["geo"] + u * dx["meridional"] + v * dy["meridional"]
            )
            t = thickness - dt * (dx["flux_x"] + dy["flux_y"])
            h = field("temp") - dt * (u * dx["temp"] + v * dy["temp"])
            z, m, t, h = (pair(misfit, (c, 0), pp) * w for c, w in enumerate((z, m, t, h)))
            for c, w in enumerate((z, m, t, h)):
                costs[(c * PROBES + probe) * 3 + pp] = w
            made = (u * z, u * m, v * z, v * m, z, m, t, u * h, v * h)
            for n, w in zip(ADJOINT, made):
                planes[n, probe, pp] = w
    put_strips(
        [planes[n, pr, pp] for n in ADJOINT for pr in range(PROBES) for pp in range(3)],
        strips,
        lax.axis_index("tx"),
    )
    put_outer_rows(
        [planes[n, pr, pp] for n in ADJOINT_X for pr in range(PROBES) for pp in range(3)],
        near_row,
        far_row,
    )


def adjoint_kernel(
    nt,
    levels,
    sides,
    row,
    swapped_a,
    swapped_b,
    costs,
    wind,
    mass,
    heat,
    backs,
    loads,
):
    west, east, south, north = outer_values(nt, sides, row, swapped_a, swapped_b)
    for pp in range(3):
        u = pair(wind, (0, 0), pp)
        v = pair(wind, (1, 0), pp)
        mass_here = pair(mass, (0,), pp)
        heat_here = pair(heat, (0,), pp)
        for probe in range(PROBES):
            z, m, t, h = (costs[(c * PROBES + probe) * 3 + pp] for c in range(4))
            field = dict(
                zip(ADJOINT, (u * z, u * m, v * z, v * m, z, m, t, u * h, v * h))
            )
            at = lambda n, k: (list(k).index(n) * PROBES + probe) * 3 + pp
            dx = {n: slopes_x(field[n], at(n, ADJOINT_X), west, east) for n in ADJOINT_X}
            dy = {n: slopes_y(field[n], at(n, ADJOINT_Y), south, north) for n in ADJOINT_Y}
            geo_back = dt * (dx["z"] + dy["m"])
            flux_x_back = dt * dx["t"]
            flux_y_back = dt * dy["t"]
            out = (
                z + dt * (dx["ez"] + dy["nz"]) + mass_here * flux_x_back,
                m + dt * (dx["em"] + dy["nm"]) + mass_here * flux_y_back,
                t + u * flux_x_back + v * flux_y_back,
                h + dt * (dx["eh"] + dy["nh"]) + geo_back,
            )
            for c, w in enumerate(out):
                backs[(c * PROBES + probe) * 3 + pp] = w
            load = heat_here * geo_back
            for k in range(levels):
                loads[k, (probe * 3 + pp) * 8 : (probe * 3 + pp) * 8 + 8] = load


def final_kernel(level_count, probes, spread, backs, loads, out):
    level = lax.axis_index("face")
    for probe in range(PROBES):
        for pp in range(3):
            at = (probe * 3 + pp) * 8
            load = jnp.zeros((8, 128), jnp.float32)
            for k in range(level_count):
                load = load + jnp.where(k >= level, loads[k, at : at + 8], 0.0)
            for c in range(4):
                back = backs[(c * PROBES + probe) * 3 + pp]
                if c == 2:
                    back = back + load
                for side in range(2):
                    part = back[:, 64 * side : 64 * side + 64]
                    p = 2 * pp + side
                    out[probe, c, 0, p] = probes[probe, c, 0, p] + spread[c, 0, p] * part


SMEM = pl.BlockSpec(memory_space=pltpu.SMEM)
VMEM = pl.BlockSpec(memory_space=pltpu.VMEM)
INTERPRET = False
GRANT = 8 << 20


def call(kernel, operands, shapes):
    shapes = [jax.ShapeDtypeStruct(s, jnp.float32) for s in shapes]
    return pl.pallas_call(
        kernel,
        out_shape=shapes,
        in_specs=[VMEM] * len(operands),
        out_specs=[VMEM] * len(shapes),
        compiler_params=pltpu.CompilerParams(vmem_limit_bytes=GRANT),
        interpret=INTERPRET,
    )(*operands)


def thickness_copies(slots, links, probes, spread):
    return pl.pallas_call(
        functools.partial(thickness_kernel, slots),
        name="thickness",
        grid=(1,),
        out_shape=[
            jax.ShapeDtypeStruct((slots, 48, 128), jnp.float32),
            jax.ShapeDtypeStruct((4, 8, 64), jnp.float32),
        ],
        in_specs=[
            SMEM,
            pl.BlockSpec((PROBES, 1, 1, 6, 8, 64), lambda i: (0, 2, 0, 0, 0, 0)),
            pl.BlockSpec((1, 1, 6, 8, 64), lambda i: (2, 0, 0, 0, 0)),
        ],
        out_specs=[
            pl.BlockSpec((slots, 48, 128), lambda i: (0, 0, 0)),
            pl.BlockSpec((4, 8, 64), lambda i: (0, 0, 0)),
        ],
        interpret=INTERPRET,
    )(links, probes, spread)


def exchange(kind, nt, nq, table, strips, near_row, far_row):
    sources, x_targets, y_targets = TABLES[kind]
    codes = jnp.asarray(codes_of(sources, x_targets, y_targets))
    picks = jnp.asarray(picks_of(sources, y_targets))
    near = [(i, i ^ 1) for i in range(nt)]
    wrapped = [(i, (i + 1 if i % 2 else i - 1) % nt) for i in range(nt)]
    swapped_a = lax.ppermute(near_row, "tx", near)
    gathered = lax.all_gather(strips, "ty", axis=0)
    slots, swap_b, local, halos = call(
        functools.partial(route_kernel, nt, nq),
        (table, gathered, far_row, codes, picks),
        ((nt, 8, 128), (32, 128), (32, 128), (16, 64)),
    )
    swapped_b = lax.ppermute(swap_b, "tx", wrapped)
    arrived = lax.all_to_all(slots, "tx", 0, 0, tiled=True)
    sides, row = call(
        functools.partial(collect_kernel, nt, nq),
        (table, arrived, local, halos),
        ((16, 128), (32, 128)),
    )
    return sides, row, swapped_a, swapped_b


def body(probes, wind, mass, heat, spread, misfit, links):
    nf, nt, nq = (lax.axis_size(a) for a in ("face", "tx", "ty"))
    sent, table = thickness_copies(nf, links, probes, spread)
    totals = lax.all_to_all(sent, "face", 0, 0, tiled=True)
    fields, strips, *rows = call(
        functools.partial(fields_kernel, nf),
        (probes, spread, wind, mass, heat, totals),
        ((36, 8, 128), (STRIP, 128), (32, 128), (32, 128)),
    )
    outer = exchange("forward", nt, nq, table, strips, *rows)
    costs, strips, *rows = call(
        functools.partial(image_kernel, nt),
        (*outer, fields, probes, spread, wind, misfit),
        ((24, 8, 128), (STRIP, 128), (32, 128), (32, 128)),
    )
    outer = exchange("adjoint", nt, nq, table, strips, *rows)
    backs, loads = call(
        functools.partial(adjoint_kernel, nt, nf),
        (*outer, costs, wind, mass, heat),
        ((24, 8, 128), (nf, 48, 128)),
    )
    loads = lax.all_to_all(loads, "face", 0, 0, tiled=True)
    (applied,) = call(
        functools.partial(final_kernel, nf), (probes, spread, backs, loads), (probes.shape,)
    )
    return applied


def solution(mesh):
    return jax.shard_map(
        body,
        mesh=mesh,
        in_specs=(
            P(None, None, "face", None, "tx", "ty"),
            P(None, "face", None, "tx", "ty"),
            P("face", None, "tx", "ty"),
            P("face", None, "tx", "ty"),
            P(None, "face", None, "tx", "ty"),
            P(None, "face", None, "tx", "ty"),
            P(),
        ),
        out_specs=P(None, None, "face", None, "tx", "ty"),
        check_vma=False,
    )
```

```python
import functools

import jax
import jax.numpy as jnp
import numpy as np
from jax import lax
from jax.experimental import pallas as pl
from jax.experimental.pallas import tpu as pltpu
from jax.sharding import PartitionSpec as P

dt = 0.3
PROBES = 2
FORWARD = ("zonal", "meridional", "flux_x", "flux_y", "temp", "geo")
FORWARD_X = {
    "geo": {"geo": (0, 0)},
    "zonal": {"zonal": (1, 0), "meridional": (2, 0)},
    "meridional": {"zonal": (3, 0), "meridional": (4, 0)},
    "flux_x": {"flux_x": (1, 0), "flux_y": (2, 0)},
    "temp": {"temp": (0, 0)},
}
FORWARD_Y = {
    "geo": {"geo": (0, 0)},
    "zonal": {"zonal": (1, 0), "meridional": (2, 0)},
    "meridional": {"zonal": (3, 0), "meridional": (4, 0)},
    "flux_y": {"flux_x": (3, 0), "flux_y": (4, 0)},
    "temp": {"temp": (0, 0)},
}
ADJOINT = ("ez", "em", "nz", "nm", "z", "m", "t", "eh", "nh")
ADJOINT_X = {
    "ez": {"ez": (1, 1), "em": (1, 2), "nz": (2, 1), "nm": (2, 2)},
    "em": {"ez": (1, 3), "em": (1, 4), "nz": (2, 3), "nm": (2, 4)},
    "z": {"z": (1, 0), "m": (2, 0)},
    "t": {"t": (0, 0)},
    "eh": {"eh": (1, 0), "nh": (2, 0)},
}
ADJOINT_Y = {
    "nz": {"ez": (3, 1), "em": (3, 2), "nz": (4, 1), "nm": (4, 2)},
    "nm": {"ez": (3, 3), "em": (3, 4), "nz": (4, 3), "nm": (4, 4)},
    "m": {"z": (3, 0), "m": (4, 0)},
    "t": {"t": (0, 0)},
    "nh": {"eh": (3, 0), "nh": (4, 0)},
}
ROWS = 56
STRIP = 16 + ROWS


def source_index(unit, panel):
    return (panel % 2) * 64 + unit * 3 + panel // 2


def target_index(unit, panel):
    return (panel % 2) * 32 + unit * 3 + panel // 2


def codes_of(sources, x_targets, y_targets):
    codes = np.full((5, 128, 64), -1.0, np.float32)
    for d, targets in enumerate((x_targets, y_targets)):
        for t, (_, terms) in enumerate(targets.items()):
            for name, (i, j) in terms.items():
                s = sources.index(name)
                for probe in range(PROBES):
                    for n in range(6):
                        for f in range(6):
                            r = source_index(s * PROBES + probe, n)
                            c = target_index(t * PROBES + probe, f)
                            codes[2 * d, r, c] = i
                            codes[2 * d + 1, r, c] = j
    for u in range(len(sources) * PROBES):
        for n in range(6):
            codes[4, source_index(u, n), :] = n
    return codes


def picks_of(sources, y_targets):
    picks = np.zeros((128, 64), np.float32)
    for t, name in enumerate(y_targets):
        for probe in range(PROBES):
            for f in range(6):
                picks[
                    source_index(sources.index(name) * PROBES + probe, f),
                    target_index(t * PROBES + probe, f),
                ] = 1.0
    return picks


TABLES = {
    "forward": (FORWARD, FORWARD_X, FORWARD_Y),
    "adjoint": (ADJOINT, ADJOINT_X, ADJOINT_Y),
}


def parts(data):
    high = data.astype(jnp.bfloat16)
    rest = data - high.astype(jnp.float32)
    middle = rest.astype(jnp.bfloat16)
    low = (rest - middle.astype(jnp.float32)).astype(jnp.bfloat16)
    return high, middle, low


def product(a, b, contract):
    return lax.dot_general(
        a,
        b,
        (((contract[0],), (contract[1],)), ((), ())),
        preferred_element_type=jnp.float32,
    )


def moved(data, choice, contract=(1, 0)):
    high, middle, low = (product(d, choice, contract) for d in data)
    return (high + middle) + low


def chosen(choice, data, contract=(1, 0)):
    high, middle, low = (product(choice, d, contract) for d in data)
    return (high + middle) + low


def reversal(size):
    row = lax.broadcasted_iota(jnp.int32, (size, size), 0)
    column = lax.broadcasted_iota(jnp.int32, (size, size), 1)
    return (row + column == size - 1).astype(jnp.float32).astype(jnp.bfloat16)


def identity(size):
    row = lax.broadcasted_iota(jnp.int32, (size, size), 0)
    column = lax.broadcasted_iota(jnp.int32, (size, size), 1)
    return (row == column).astype(jnp.float32).astype(jnp.bfloat16)


def lanes(shape):
    return lax.broadcasted_iota(jnp.int32, shape, len(shape) - 1)


def joined(even, odd):
    return jnp.concatenate([even, odd], axis=1)


def joined_all(pieces):
    return jnp.concatenate(pieces, axis=1)


def pair(ref, index, pp):
    return joined(ref[(*index, 2 * pp)], ref[(*index, 2 * pp + 1)])


def put_table(links, table):
    lane = lanes((1, 64))
    within = jnp.where(lane >= 32, lane - 32, lane)
    third = within - 3 * ((within * 43) // 128)
    here = [(third == f // 2) & ((lane >= 32) == (f % 2 == 1)) for f in range(6)]
    for edge in range(4):
        for item in range(7):
            out = jnp.zeros((1, 64), jnp.float32)
            for f in range(6):
                out = jnp.where(here[f], links[f, edge, item].astype(jnp.float32), out)
            table[edge, item : item + 1] = out
        table[edge, 7:8] = jnp.zeros((1, 64), jnp.float32)


def link_lanes(table, edge, item):
    return table[edge, item : item + 1]


def coefficients(links, edge, code_a, code_b, panel):
    one = jnp.ones((1, 64), jnp.float32)
    entries = [one] + [link_lanes(links, edge, 3 + k) for k in range(4)]
    a = jnp.zeros(code_a.shape, jnp.float32)
    b = jnp.zeros(code_a.shape, jnp.float32)
    for k in range(5):
        a = jnp.where(code_a == k, entries[k], a)
        b = jnp.where(code_b == k, entries[k], b)
    return jnp.where(panel == link_lanes(links, edge, 0), a * b, 0.0)


def put_strips(planes, out_ref, tile_row):
    lane = lanes((8, 128))
    south = jnp.zeros((8, 128), jnp.float32)
    north = jnp.zeros((8, 128), jnp.float32)
    rows = []
    for a, plane in enumerate(planes):
        here = (lane == a) | (lane == a + 64)
        south = jnp.where(here, plane if a == 0 else pltpu.roll(plane, a, 1), south)
        shift = (a - 63) % 128
        north = jnp.where(here, plane if shift == 0 else pltpu.roll(plane, shift, 1), north)
        rows.append(jnp.where(tile_row == 0, plane[0:1], plane[7:8]))
    out_ref[0:8] = south
    out_ref[8:16] = north
    rows.append(jnp.zeros((ROWS - len(rows), 128), jnp.float32))
    out_ref[16:STRIP] = jnp.concatenate(rows, axis=0)


def put_outer_rows(planes, near_ref, far_ref):
    spare = [jnp.zeros((32 - len(planes), 128), jnp.float32)]
    top = jnp.concatenate([p[0:1] for p in planes] + spare, axis=0)
    bottom = jnp.concatenate([p[7:8] for p in planes] + spare, axis=0)
    even = lax.rem(lax.axis_index("tx"), 2) == 0
    near_ref[...] = jnp.where(even, bottom, top)
    far_ref[...] = jnp.where(even, top, bottom)


def slopes_x(plane, b, west, east):
    row = lax.broadcasted_iota(jnp.int32, (8, 128), 0)
    after = jnp.where(row == 7, east[b : b + 1], pltpu.roll(plane, 7, 0))
    before = jnp.where(row == 0, west[b : b + 1], pltpu.roll(plane, 1, 0))
    return 0.5 * (after - before)


def slopes_y(plane, b, south, north):
    lane = lanes((8, 128))
    low = (lane == 0) | (lane == 64)
    high = (lane == 63) | (lane == 127)
    from_south = south if b == 0 else pltpu.roll(south, 128 - b, 1)
    after = jnp.where(high, pltpu.roll(north, 63 - b, 1), pltpu.roll(plane, 127, 1))
    before = jnp.where(low, from_south, pltpu.roll(plane, 1, 1))
    return 0.5 * (after - before)


def thickness_kernel(slots, links, probes, spread, out, table):
    put_table(links, table)
    for probe in range(PROBES):
        for pp in range(3):
            value = pair(spread, (0, 0), pp) * pair(probes, (probe, 0, 0), pp)
            for k in range(slots):
                out[k, (probe * 3 + pp) * 8 : (probe * 3 + pp) * 8 + 8] = value


def fields_kernel(
    level_count,
    probes,
    spread,
    wind,
    mass,
    heat,
    misfit,
    totals,
    fields,
    strips,
    near_row,
    far_row,
    weights,
):
    level, tile_row = lax.axis_index("face"), lax.axis_index("tx")
    planes = {}
    for pp in range(3):
        east = pair(wind, (0, 0), pp)
        north = pair(wind, (1, 0), pp)
        mass_here = pair(mass, (0,), pp)
        heat_here = pair(heat, (0,), pp)
        for c in range(4):
            weights[c * 3 + pp] = pair(misfit, (c, 0), pp)
        for probe in range(PROBES):
            scaled = [
                pair(spread, (c, 0), pp) * pair(probes, (probe, c, 0), pp) for c in range(4)
            ]
            zonal, meridional, thickness, temp = scaled
            at = (probe * 3 + pp) * 8
            pressure = thickness
            for k in range(level_count - 1):
                pressure = pressure + jnp.where(k < level, totals[k, at : at + 8], 0.0)
            planes["zonal", probe, pp] = zonal
            planes["meridional", probe, pp] = meridional
            planes["flux_x", probe, pp] = east * thickness + mass_here * zonal
            planes["flux_y", probe, pp] = north * thickness + mass_here * meridional
            planes["temp", probe, pp] = temp
            planes["geo", probe, pp] = temp + heat_here * pressure
    ordered = [planes[n, pr, pp] for n in FORWARD for pr in range(PROBES) for pp in range(3)]
    for a, plane in enumerate(ordered):
        fields[a] = plane
    put_strips(ordered, strips, tile_row)
    put_outer_rows(
        [planes[n, pr, pp] for n in FORWARD_X for pr in range(PROBES) for pp in range(3)],
        near_row,
        far_row,
    )


def route_kernel(
    nt, nq, links, gathered, far_row, codes, picks, slots, swap_b, local, halos
):
    tile_row, tile_column = lax.axis_index("tx"), lax.axis_index("ty")
    is_first, is_last = tile_row == 0, tile_row == nt - 1
    line_f = jnp.where(is_first, 0.0, 1.0)
    column_edge = jnp.where(tile_column == 0, 2, 3)
    panel = codes[4]
    c0 = coefficients(links, 0, codes[0], codes[1], panel)
    c1 = coefficients(links, 1, codes[0], codes[1], panel)
    cc = coefficients(links, column_edge, codes[2], codes[3], panel)
    ends = joined(c0, c1).astype(jnp.bfloat16)
    cc = cc.astype(jnp.bfloat16)

    def masks(edge, source):
        far = link_lanes(links, edge, 1)
        flip = link_lanes(links, edge, 2)
        here = far == source
        return (
            jnp.where(here & (flip != 1.0), 1.0, 0.0),
            jnp.where(here & (flip == 1.0), 1.0, 0.0),
        )

    back64 = reversal(64)
    empty = jnp.zeros((64 - ROWS, 64), jnp.float32)

    def segment(q):
        packed = gathered[q, 16:STRIP]
        return parts(
            jnp.concatenate([packed[:, 0:64], empty, packed[:, 64:128], empty], axis=0)
        )

    on_boundary = jnp.where(is_first | is_last, 1.0, 0.0)
    plain_c, turned_c = masks(column_edge, line_f)
    across = [moved(segment(q), cc, (0, 0)) * on_boundary for q in range(nq)]
    turned = joined_all([a * turned_c for a in across])
    turned = chosen(back64, parts(turned))
    pieces = [
        across[q] * plain_c + turned[:, 64 * (nq - 1 - q) : 64 * (nq - q)] for q in range(nq)
    ]
    columns = parts(jnp.concatenate([gathered[0, 0:8], gathered[nq - 1, 8:16]], axis=0))
    low_plain, low_turned = masks(column_edge, 2.0)
    high_plain, high_turned = masks(column_edge, 3.0)
    to_columns = moved(columns, cc)
    low_c, high_c = to_columns[0:8], to_columns[8:16]
    straight = low_c * low_plain + high_c * high_plain
    flipped = chosen(reversal(8), parts(low_c * low_turned + high_c * high_turned))
    to_rows = moved(columns, ends)
    far = joined(link_lanes(links, 0, 1), link_lanes(links, 1, 1))
    to_rows = to_rows[0:8] * jnp.where(far == 2.0, 1.0, 0.0) + to_rows[8:16] * jnp.where(
        far == 3.0, 1.0, 0.0
    )
    to_rows = [to_rows[:, 0:64], to_rows[:, 64:128]]
    for t in range(nt):
        q, at = t // 8, (t % 8) * 8
        left = pieces[q][at : at + 8]
        left = left + jnp.where(tile_row == t, straight, 0.0)
        left = left + jnp.where(tile_row == nt - 1 - t, flipped, 0.0)
        slots[t] = joined(left, to_rows[1] if t == nt - 1 else to_rows[0])

    plain0, turned0 = masks(0, line_f)
    plain1, turned1 = masks(1, line_f)
    plain = (joined(c0, c1) * joined(plain0, plain1)).astype(jnp.bfloat16)
    mirror = (joined(c0, c1) * joined(turned0, turned1)).astype(jnp.bfloat16)
    by_row = chosen(plain, segment(tile_column), (0, 0))
    by_row = by_row + moved(
        parts(chosen(mirror, segment(nq - 1 - tile_column), (0, 0))), back64
    )
    by_row = [joined(by_row[k : k + 32], by_row[k + 32 : k + 64]) for k in (0, 64)]
    local[...] = jnp.where(is_first, by_row[0], by_row[1])
    sent = jnp.where(is_first, by_row[1], far_row[...])
    swap_b[...] = jnp.where(is_last, by_row[0], sent)

    below = gathered[jnp.maximum(tile_column - 1, 0), 8:16]
    above = gathered[jnp.minimum(tile_column + 1, nq - 1), 0:8]
    near = moved(parts(jnp.concatenate([below, above], axis=0)), picks[...].astype(jnp.bfloat16))
    halos[0:8] = jnp.where(tile_column > 0, near[0:8], 0.0)
    halos[8:16] = jnp.where(tile_column < nq - 1, near[8:16], 0.0)


def collect_kernel(nt, nq, links, arrived, local, halos, sides, row_out):
    tile_row, tile_column = lax.axis_index("tx"), lax.axis_index("ty")
    is_first, is_last = tile_row == 0, tile_row == nt - 1
    column = arrived[0]
    for t in range(1, nt):
        column = column + arrived[t]
    column = column[:, 0:64]
    lane = lanes((8, 128))

    def spread_out(narrow):
        wide = joined(narrow, narrow)
        return jnp.where(lane < 32, wide, pltpu.roll(wide, 32, 1))

    sides[0:8] = spread_out(halos[0:8] + jnp.where(tile_column == 0, column, 0.0))
    sides[8:16] = spread_out(halos[8:16] + jnp.where(tile_column == nq - 1, column, 0.0))
    mine = arrived[pl.ds(tile_column * 8, 8)].reshape(64, 128)[:, 64:128]
    mirrored = arrived[pl.ds((nq - 1 - tile_column) * 8, 8)].reshape(64, 128)[:, 64:128]
    flip = link_lanes(links, jnp.where(is_first, 0, 1), 2)
    row = moved(parts(jnp.where(flip != 1.0, mine, 0.0)), identity(64), (0, 0)) + moved(
        parts(jnp.where(flip == 1.0, mirrored, 0.0)), reversal(64), (0, 0)
    )
    row_out[...] = joined(row[0:32], row[32:64]) + local[...]


def outer_values(nt, sides, row, swapped_a, swapped_b):
    tile_row = lax.axis_index("tx")
    even = lax.rem(tile_row, 2) == 0
    west = jnp.where(even, swapped_b[...], swapped_a[...])
    east = jnp.where(even, swapped_a[...], swapped_b[...])
    west = west + jnp.where(tile_row == 0, row[...], 0.0)
    east = east + jnp.where(tile_row == nt - 1, row[...], 0.0)
    return west, east, sides[0:8], sides[8:16]


def image_kernel(
    nt,
    sides,
    row,
    swapped_a,
    swapped_b,
    fields,
    probes,
    spread,
    wind,
    weights,
    costs,
    strips,
    near_row,
    far_row,
):
    west, east, south, north = outer_values(nt, sides, row, swapped_a, swapped_b)
    planes = {}
    for pp in range(3):
        u = pair(wind, (0, 0), pp)
        v = pair(wind, (1, 0), pp)
        for probe in range(PROBES):
            field = lambda n: fields[(FORWARD.index(n) * PROBES + probe) * 3 + pp]
            at = lambda n, t: (list(t).index(n) * PROBES + probe) * 3 + pp
            dx = {n: slopes_x(field(n), at(n, FORWARD_X), west, east) for n in FORWARD_X}
            dy = {n: slopes_y(field(n), at(n, FORWARD_Y), south, north) for n in FORWARD_Y}
            thickness = pair(spread, (2, 0), pp) * pair(probes, (probe, 2, 0), pp)
            z = field("zonal") - dt * (dx["geo"] + u * dx["zonal"] + v * dy["zonal"])
            m = field("meridional") - dt * (
                dy["geo"] + u * dx["meridional"] + v * dy["meridional"]
            )
            t = thickness - dt * (dx["flux_x"] + dy["flux_y"])
            h = field("temp") - dt * (u * dx["temp"] + v * dy["temp"])
            z, m, t, h = (weights[c * 3 + pp] * w for c, w in enumerate((z, m, t, h)))
            for c, w in enumerate((z, m, t, h)):
                costs[(c * PROBES + probe) * 3 + pp] = w
            made = (u * z, u * m, v * z, v * m, z, m, t, u * h, v * h)
            for n, w in zip(ADJOINT, made):
                planes[n, probe, pp] = w
    put_strips(
        [planes[n, pr, pp] for n in ADJOINT for pr in range(PROBES) for pp in range(3)],
        strips,
        lax.axis_index("tx"),
    )
    put_outer_rows(
        [planes[n, pr, pp] for n in ADJOINT_X for pr in range(PROBES) for pp in range(3)],
        near_row,
        far_row,
    )


def adjoint_kernel(
    nt,
    levels,
    sides,
    row,
    swapped_a,
    swapped_b,
    costs,
    wind,
    mass,
    heat,
    backs,
    loads,
):
    west, east, south, north = outer_values(nt, sides, row, swapped_a, swapped_b)
    for pp in range(3):
        u = pair(wind, (0, 0), pp)
        v = pair(wind, (1, 0), pp)
        mass_here = pair(mass, (0,), pp)
        heat_here = pair(heat, (0,), pp)
        for probe in range(PROBES):
            z, m, t, h = (costs[(c * PROBES + probe) * 3 + pp] for c in range(4))
            field = dict(
                zip(ADJOINT, (u * z, u * m, v * z, v * m, z, m, t, u * h, v * h))
            )
            at = lambda n, k: (list(k).index(n) * PROBES + probe) * 3 + pp
            dx = {n: slopes_x(field[n], at(n, ADJOINT_X), west, east) for n in ADJOINT_X}
            dy = {n: slopes_y(field[n], at(n, ADJOINT_Y), south, north) for n in ADJOINT_Y}
            geo_back = dt * (dx["z"] + dy["m"])
            flux_x_back = dt * dx["t"]
            flux_y_back = dt * dy["t"]
            out = (
                z + dt * (dx["ez"] + dy["nz"]) + mass_here * flux_x_back,
                m + dt * (dx["em"] + dy["nm"]) + mass_here * flux_y_back,
                t + u * flux_x_back + v * flux_y_back,
                h + dt * (dx["eh"] + dy["nh"]) + geo_back,
            )
            for c, w in enumerate(out):
                backs[(c * PROBES + probe) * 3 + pp] = w
            load = heat_here * geo_back
            for k in range(levels):
                loads[k, (probe * 3 + pp) * 8 : (probe * 3 + pp) * 8 + 8] = load


def final_kernel(level_count, probes, spread, backs, loads, out):
    level = lax.axis_index("face")
    for probe in range(PROBES):
        for pp in range(3):
            at = (probe * 3 + pp) * 8
            load = jnp.zeros((8, 128), jnp.float32)
            for k in range(level_count):
                load = load + jnp.where(k >= level, loads[k, at : at + 8], 0.0)
            for c in range(4):
                back = backs[(c * PROBES + probe) * 3 + pp]
                if c == 2:
                    back = back + load
                for side in range(2):
                    part = back[:, 64 * side : 64 * side + 64]
                    p = 2 * pp + side
                    out[probe, c, 0, p] = probes[probe, c, 0, p] + spread[c, 0, p] * part


SMEM = pl.BlockSpec(memory_space=pltpu.SMEM)
VMEM = pl.BlockSpec(memory_space=pltpu.VMEM)
INTERPRET = False
GRANT = 8 << 20


def call(kernel, operands, shapes):
    shapes = [jax.ShapeDtypeStruct(s, jnp.float32) for s in shapes]
    return pl.pallas_call(
        kernel,
        out_shape=shapes,
        in_specs=[VMEM] * len(operands),
        out_specs=[VMEM] * len(shapes),
        compiler_params=pltpu.CompilerParams(vmem_limit_bytes=GRANT),
        interpret=INTERPRET,
    )(*operands)


def thickness_copies(slots, links, probes, spread):
    return pl.pallas_call(
        functools.partial(thickness_kernel, slots),
        name="thickness",
        grid=(1,),
        out_shape=[
            jax.ShapeDtypeStruct((slots, 48, 128), jnp.float32),
            jax.ShapeDtypeStruct((4, 8, 64), jnp.float32),
        ],
        in_specs=[
            SMEM,
            pl.BlockSpec((PROBES, 1, 1, 6, 8, 64), lambda i: (0, 2, 0, 0, 0, 0)),
            pl.BlockSpec((1, 1, 6, 8, 64), lambda i: (2, 0, 0, 0, 0)),
        ],
        out_specs=[
            pl.BlockSpec((slots, 48, 128), lambda i: (0, 0, 0)),
            pl.BlockSpec((4, 8, 64), lambda i: (0, 0, 0)),
        ],
        interpret=INTERPRET,
    )(links, probes, spread)


def exchange(kind, nt, nq, table, strips, near_row, far_row):
    sources, x_targets, y_targets = TABLES[kind]
    codes = jnp.asarray(codes_of(sources, x_targets, y_targets))
    picks = jnp.asarray(picks_of(sources, y_targets))
    near = [(i, i ^ 1) for i in range(nt)]
    wrapped = [(i, (i + 1 if i % 2 else i - 1) % nt) for i in range(nt)]
    swapped_a = lax.ppermute(near_row, "tx", near)
    gathered = lax.all_gather(strips, "ty", axis=0)
    slots, swap_b, local, halos = call(
        functools.partial(route_kernel, nt, nq),
        (table, gathered, far_row, codes, picks),
        ((nt, 8, 128), (32, 128), (32, 128), (16, 64)),
    )
    swapped_b = lax.ppermute(swap_b, "tx", wrapped)
    arrived = lax.all_to_all(slots, "tx", 0, 0, tiled=True)
    sides, row = call(
        functools.partial(collect_kernel, nt, nq),
        (table, arrived, local, halos),
        ((16, 128), (32, 128)),
    )
    return sides, row, swapped_a, swapped_b


def body(probes, wind, mass, heat, spread, misfit, links):
    nf, nt, nq = (lax.axis_size(a) for a in ("face", "tx", "ty"))
    sent, table = thickness_copies(nf, links, probes, spread)
    totals = lax.all_to_all(sent, "face", 0, 0, tiled=True)
    fields, strips, *rows, weights = call(
        functools.partial(fields_kernel, nf),
        (probes, spread, wind, mass, heat, misfit, totals),
        ((36, 8, 128), (STRIP, 128), (32, 128), (32, 128), (12, 8, 128)),
    )
    outer = exchange("forward", nt, nq, table, strips, *rows)
    costs, strips, *rows = call(
        functools.partial(image_kernel, nt),
        (*outer, fields, probes, spread, wind, weights),
        ((24, 8, 128), (STRIP, 128), (32, 128), (32, 128)),
    )
    outer = exchange("adjoint", nt, nq, table, strips, *rows)
    backs, loads = call(
        functools.partial(adjoint_kernel, nt, nf),
        (*outer, costs, wind, mass, heat),
        ((24, 8, 128), (nf, 48, 128)),
    )
    loads = lax.all_to_all(loads, "face", 0, 0, tiled=True)
    (applied,) = call(
        functools.partial(final_kernel, nf), (probes, spread, backs, loads), (probes.shape,)
    )
    return applied


def solution(mesh):
    return jax.shard_map(
        body,
        mesh=mesh,
        in_specs=(
            P(None, None, "face", None, "tx", "ty"),
            P(None, "face", None, "tx", "ty"),
            P("face", None, "tx", "ty"),
            P("face", None, "tx", "ty"),
            P(None, "face", None, "tx", "ty"),
            P(None, "face", None, "tx", "ty"),
            P(),
        ),
        out_specs=P(None, None, "face", None, "tx", "ty"),
        check_vma=False,
    )
```

```python
import functools

import jax
import jax.numpy as jnp
import numpy as np
from jax import lax
from jax.experimental import pallas as pl
from jax.experimental.pallas import tpu as pltpu
from jax.sharding import PartitionSpec as P

dt = 0.3
PROBES = 2
FORWARD = ("zonal", "meridional", "flux_x", "flux_y", "temp", "geo")
FORWARD_X = {
    "geo": {"geo": (0, 0)},
    "zonal": {"zonal": (1, 0), "meridional": (2, 0)},
    "meridional": {"zonal": (3, 0), "meridional": (4, 0)},
    "flux_x": {"flux_x": (1, 0), "flux_y": (2, 0)},
    "temp": {"temp": (0, 0)},
}
FORWARD_Y = {
    "geo": {"geo": (0, 0)},
    "zonal": {"zonal": (1, 0), "meridional": (2, 0)},
    "meridional": {"zonal": (3, 0), "meridional": (4, 0)},
    "flux_y": {"flux_x": (3, 0), "flux_y": (4, 0)},
    "temp": {"temp": (0, 0)},
}
ADJOINT = ("ez", "em", "nz", "nm", "z", "m", "t", "eh", "nh")
ADJOINT_X = {
    "ez": {"ez": (1, 1), "em": (1, 2), "nz": (2, 1), "nm": (2, 2)},
    "em": {"ez": (1, 3), "em": (1, 4), "nz": (2, 3), "nm": (2, 4)},
    "z": {"z": (1, 0), "m": (2, 0)},
    "t": {"t": (0, 0)},
    "eh": {"eh": (1, 0), "nh": (2, 0)},
}
ADJOINT_Y = {
    "nz": {"ez": (3, 1), "em": (3, 2), "nz": (4, 1), "nm": (4, 2)},
    "nm": {"ez": (3, 3), "em": (3, 4), "nz": (4, 3), "nm": (4, 4)},
    "m": {"z": (3, 0), "m": (4, 0)},
    "t": {"t": (0, 0)},
    "nh": {"eh": (3, 0), "nh": (4, 0)},
}
ROWS = 56
STRIP = 16 + ROWS


def source_index(unit, panel):
    return (panel % 2) * 64 + unit * 3 + panel // 2


def target_index(unit, panel):
    return (panel % 2) * 32 + unit * 3 + panel // 2


def codes_of(sources, x_targets, y_targets):
    codes = np.full((5, 128, 64), -1.0, np.float32)
    for d, targets in enumerate((x_targets, y_targets)):
        for t, (_, terms) in enumerate(targets.items()):
            for name, (i, j) in terms.items():
                s = sources.index(name)
                for probe in range(PROBES):
                    for n in range(6):
                        for f in range(6):
                            r = source_index(s * PROBES + probe, n)
                            c = target_index(t * PROBES + probe, f)
                            codes[2 * d, r, c] = i
                            codes[2 * d + 1, r, c] = j
    for u in range(len(sources) * PROBES):
        for n in range(6):
            codes[4, source_index(u, n), :] = n
    return codes


def picks_of(sources, y_targets):
    picks = np.zeros((128, 64), np.float32)
    for t, name in enumerate(y_targets):
        for probe in range(PROBES):
            for f in range(6):
                picks[
                    source_index(sources.index(name) * PROBES + probe, f),
                    target_index(t * PROBES + probe, f),
                ] = 1.0
    return picks


TABLES = {
    "forward": (FORWARD, FORWARD_X, FORWARD_Y),
    "adjoint": (ADJOINT, ADJOINT_X, ADJOINT_Y),
}


def parts(data):
    high = data.astype(jnp.bfloat16)
    rest = data - high.astype(jnp.float32)
    middle = rest.astype(jnp.bfloat16)
    low = (rest - middle.astype(jnp.float32)).astype(jnp.bfloat16)
    return high, middle, low


def product(a, b, contract):
    return lax.dot_general(
        a,
        b,
        (((contract[0],), (contract[1],)), ((), ())),
        preferred_element_type=jnp.float32,
    )


def moved(data, choice, contract=(1, 0)):
    high, middle, low = (product(d, choice, contract) for d in data)
    return (high + middle) + low


def chosen(choice, data, contract=(1, 0)):
    high, middle, low = (product(choice, d, contract) for d in data)
    return (high + middle) + low


def reversal(size):
    row = lax.broadcasted_iota(jnp.int32, (size, size), 0)
    column = lax.broadcasted_iota(jnp.int32, (size, size), 1)
    return (row + column == size - 1).astype(jnp.float32).astype(jnp.bfloat16)


def identity(size):
    row = lax.broadcasted_iota(jnp.int32, (size, size), 0)
    column = lax.broadcasted_iota(jnp.int32, (size, size), 1)
    return (row == column).astype(jnp.float32).astype(jnp.bfloat16)


def lanes(shape):
    return lax.broadcasted_iota(jnp.int32, shape, len(shape) - 1)


def joined(even, odd):
    return jnp.concatenate([even, odd], axis=1)


def joined_all(pieces):
    return jnp.concatenate(pieces, axis=1)


def pair(ref, index, pp):
    return joined(ref[(*index, 2 * pp)], ref[(*index, 2 * pp + 1)])


def put_table(links, table):
    lane = lanes((1, 64))
    within = jnp.where(lane >= 32, lane - 32, lane)
    third = within - 3 * ((within * 43) // 128)
    here = [(third == f // 2) & ((lane >= 32) == (f % 2 == 1)) for f in range(6)]
    for edge in range(4):
        for item in range(7):
            out = jnp.zeros((1, 64), jnp.float32)
            for f in range(6):
                out = jnp.where(here[f], links[f, edge, item].astype(jnp.float32), out)
            table[edge, item : item + 1] = out
        table[edge, 7:8] = jnp.zeros((1, 64), jnp.float32)


def link_lanes(table, edge, item):
    return table[edge, item : item + 1]


def coefficients(links, edge, code_a, code_b, panel):
    one = jnp.ones((1, 64), jnp.float32)
    entries = [one] + [link_lanes(links, edge, 3 + k) for k in range(4)]
    a = jnp.zeros(code_a.shape, jnp.float32)
    b = jnp.zeros(code_a.shape, jnp.float32)
    for k in range(5):
        a = jnp.where(code_a == k, entries[k], a)
        b = jnp.where(code_b == k, entries[k], b)
    return jnp.where(panel == link_lanes(links, edge, 0), a * b, 0.0)


def put_strips(planes, out_ref, tile_row):
    lane = lanes((8, 128))
    south = jnp.zeros((8, 128), jnp.float32)
    north = jnp.zeros((8, 128), jnp.float32)
    rows = []
    for a, plane in enumerate(planes):
        here = (lane == a) | (lane == a + 64)
        south = jnp.where(here, plane if a == 0 else pltpu.roll(plane, a, 1), south)
        shift = (a - 63) % 128
        north = jnp.where(here, plane if shift == 0 else pltpu.roll(plane, shift, 1), north)
        rows.append(jnp.where(tile_row == 0, plane[0:1], plane[7:8]))
    out_ref[0:8] = south
    out_ref[8:16] = north
    rows.append(jnp.zeros((ROWS - len(rows), 128), jnp.float32))
    out_ref[16:STRIP] = jnp.concatenate(rows, axis=0)


def put_outer_rows(planes, near_ref, far_ref):
    spare = [jnp.zeros((32 - len(planes), 128), jnp.float32)]
    top = jnp.concatenate([p[0:1] for p in planes] + spare, axis=0)
    bottom = jnp.concatenate([p[7:8] for p in planes] + spare, axis=0)
    even = lax.rem(lax.axis_index("tx"), 2) == 0
    near_ref[...] = jnp.where(even, bottom, top)
    far_ref[...] = jnp.where(even, top, bottom)


def slopes_x(plane, b, west, east):
    row = lax.broadcasted_iota(jnp.int32, (8, 128), 0)
    after = jnp.where(row == 7, east[b : b + 1], pltpu.roll(plane, 7, 0))
    before = jnp.where(row == 0, west[b : b + 1], pltpu.roll(plane, 1, 0))
    return 0.5 * (after - before)


def slopes_y(plane, b, south, north):
    lane = lanes((8, 128))
    low = (lane == 0) | (lane == 64)
    high = (lane == 63) | (lane == 127)
    from_south = south if b == 0 else pltpu.roll(south, 128 - b, 1)
    after = jnp.where(high, pltpu.roll(north, 63 - b, 1), pltpu.roll(plane, 127, 1))
    before = jnp.where(low, from_south, pltpu.roll(plane, 1, 1))
    return 0.5 * (after - before)


def thickness_kernel(slots, links, probes, spread, out, table):
    put_table(links, table)
    for probe in range(PROBES):
        for pp in range(3):
            value = pair(spread, (0, 0), pp) * pair(probes, (probe, 0, 0), pp)
            for k in range(slots):
                out[k, (probe * 3 + pp) * 8 : (probe * 3 + pp) * 8 + 8] = value


def fields_kernel(
    level_count,
    probes,
    spread,
    wind,
    mass,
    heat,
    misfit,
    totals,
    fields,
    strips,
    near_row,
    far_row,
    weights,
):
    level, tile_row = lax.axis_index("face"), lax.axis_index("tx")
    planes = {}
    for pp in range(3):
        east = pair(wind, (0, 0), pp)
        north = pair(wind, (1, 0), pp)
        mass_here = pair(mass, (0,), pp)
        heat_here = pair(heat, (0,), pp)
        for c in range(4):
            weights[c * 3 + pp] = pair(misfit, (c, 0), pp)
        for probe in range(PROBES):
            scaled = [
                pair(spread, (c, 0), pp) * pair(probes, (probe, c, 0), pp) for c in range(4)
            ]
            zonal, meridional, thickness, temp = scaled
            at = (probe * 3 + pp) * 8
            pressure = thickness
            for k in range(level_count - 1):
                pressure = pressure + jnp.where(k < level, totals[k, at : at + 8], 0.0)
            planes["zonal", probe, pp] = zonal
            planes["meridional", probe, pp] = meridional
            planes["flux_x", probe, pp] = east * thickness + mass_here * zonal
            planes["flux_y", probe, pp] = north * thickness + mass_here * meridional
            planes["temp", probe, pp] = temp
            planes["geo", probe, pp] = temp + heat_here * pressure
    ordered = [planes[n, pr, pp] for n in FORWARD for pr in range(PROBES) for pp in range(3)]
    for a, plane in enumerate(ordered):
        fields[a] = plane
    put_strips(ordered, strips, tile_row)
    put_outer_rows(
        [planes[n, pr, pp] for n in FORWARD_X for pr in range(PROBES) for pp in range(3)],
        near_row,
        far_row,
    )


def edge_masks(table, edge, source):
    flip = link_lanes(table, edge, 2)
    here = link_lanes(table, edge, 1) == source
    return (
        jnp.where(here & (flip != 1.0), 1.0, 0.0),
        jnp.where(here & (flip == 1.0), 1.0, 0.0),
    )


def segment(gathered, q):
    packed = gathered[q, 16:STRIP]
    empty = jnp.zeros((64 - ROWS, 64), jnp.float32)
    return parts(jnp.concatenate([packed[:, 0:64], empty, packed[:, 64:128], empty], axis=0))


def slots_kernel(nt, nq, table, gathered, codes, slots):
    tile_row, tile_column = lax.axis_index("tx"), lax.axis_index("ty")
    is_first, is_last = tile_row == 0, tile_row == nt - 1
    line_f = jnp.where(is_first, 0.0, 1.0)
    column_edge = jnp.where(tile_column == 0, 2, 3)
    panel = codes[4]
    c0 = coefficients(table, 0, codes[0], codes[1], panel)
    c1 = coefficients(table, 1, codes[0], codes[1], panel)
    cc = coefficients(table, column_edge, codes[2], codes[3], panel)
    ends = joined(c0, c1).astype(jnp.bfloat16)
    cc = cc.astype(jnp.bfloat16)
    on_boundary = jnp.where(is_first | is_last, 1.0, 0.0)
    plain_c, turned_c = edge_masks(table, column_edge, line_f)
    across = [moved(segment(gathered, q), cc, (0, 0)) * on_boundary for q in range(nq)]
    turned = joined_all([a * turned_c for a in across])
    turned = chosen(reversal(64), parts(turned))
    pieces = [
        across[q] * plain_c + turned[:, 64 * (nq - 1 - q) : 64 * (nq - q)] for q in range(nq)
    ]
    columns = parts(jnp.concatenate([gathered[0, 0:8], gathered[nq - 1, 8:16]], axis=0))
    low_plain, low_turned = edge_masks(table, column_edge, 2.0)
    high_plain, high_turned = edge_masks(table, column_edge, 3.0)
    to_columns = moved(columns, cc)
    low_c, high_c = to_columns[0:8], to_columns[8:16]
    straight = low_c * low_plain + high_c * high_plain
    flipped = chosen(reversal(8), parts(low_c * low_turned + high_c * high_turned))
    to_rows = moved(columns, ends)
    far = joined(link_lanes(table, 0, 1), link_lanes(table, 1, 1))
    to_rows = to_rows[0:8] * jnp.where(far == 2.0, 1.0, 0.0) + to_rows[8:16] * jnp.where(
        far == 3.0, 1.0, 0.0
    )
    to_rows = [to_rows[:, 0:64], to_rows[:, 64:128]]
    for t in range(nt):
        q, at = t // 8, (t % 8) * 8
        left = pieces[q][at : at + 8]
        left = left + jnp.where(tile_row == t, straight, 0.0)
        left = left + jnp.where(tile_row == nt - 1 - t, flipped, 0.0)
        slots[t] = joined(left, to_rows[1] if t == nt - 1 else to_rows[0])


def rows_kernel(nt, nq, table, gathered, far_row, codes, picks, swap_b, local, halos):
    tile_row, tile_column = lax.axis_index("tx"), lax.axis_index("ty")
    is_first, is_last = tile_row == 0, tile_row == nt - 1
    line_f = jnp.where(is_first, 0.0, 1.0)
    panel = codes[4]
    c0 = coefficients(table, 0, codes[0], codes[1], panel)
    c1 = coefficients(table, 1, codes[0], codes[1], panel)
    plain0, turned0 = edge_masks(table, 0, line_f)
    plain1, turned1 = edge_masks(table, 1, line_f)
    plain = (joined(c0, c1) * joined(plain0, plain1)).astype(jnp.bfloat16)
    mirror = (joined(c0, c1) * joined(turned0, turned1)).astype(jnp.bfloat16)
    by_row = chosen(plain, segment(gathered, tile_column), (0, 0))
    mirrored = chosen(mirror, segment(gathered, nq - 1 - tile_column), (0, 0))
    by_row = by_row + moved(parts(mirrored), reversal(64))
    by_row = [joined(by_row[k : k + 32], by_row[k + 32 : k + 64]) for k in (0, 64)]
    local[...] = jnp.where(is_first, by_row[0], by_row[1])
    sent = jnp.where(is_first, by_row[1], far_row[...])
    swap_b[...] = jnp.where(is_last, by_row[0], sent)
    below = gathered[jnp.maximum(tile_column - 1, 0), 8:16]
    above = gathered[jnp.minimum(tile_column + 1, nq - 1), 0:8]
    near = moved(parts(jnp.concatenate([below, above], axis=0)), picks[...].astype(jnp.bfloat16))
    halos[0:8] = jnp.where(tile_column > 0, near[0:8], 0.0)
    halos[8:16] = jnp.where(tile_column < nq - 1, near[8:16], 0.0)


def collect_kernel(nt, nq, links, arrived, local, halos, sides, row_out):
    tile_row, tile_column = lax.axis_index("tx"), lax.axis_index("ty")
    is_first, is_last = tile_row == 0, tile_row == nt - 1
    column = arrived[0]
    for t in range(1, nt):
        column = column + arrived[t]
    column = column[:, 0:64]
    lane = lanes((8, 128))

    def spread_out(narrow):
        wide = joined(narrow, narrow)
        return jnp.where(lane < 32, wide, pltpu.roll(wide, 32, 1))

    sides[0:8] = spread_out(halos[0:8] + jnp.where(tile_column == 0, column, 0.0))
    sides[8:16] = spread_out(halos[8:16] + jnp.where(tile_column == nq - 1, column, 0.0))
    mine = arrived[pl.ds(tile_column * 8, 8)].reshape(64, 128)[:, 64:128]
    mirrored = arrived[pl.ds((nq - 1 - tile_column) * 8, 8)].reshape(64, 128)[:, 64:128]
    flip = link_lanes(links, jnp.where(is_first, 0, 1), 2)
    row = moved(parts(jnp.where(flip != 1.0, mine, 0.0)), identity(64), (0, 0)) + moved(
        parts(jnp.where(flip == 1.0, mirrored, 0.0)), reversal(64), (0, 0)
    )
    row_out[...] = joined(row[0:32], row[32:64]) + local[...]


def outer_values(nt, sides, row, swapped_a, swapped_b):
    tile_row = lax.axis_index("tx")
    even = lax.rem(tile_row, 2) == 0
    west = jnp.where(even, swapped_b[...], swapped_a[...])
    east = jnp.where(even, swapped_a[...], swapped_b[...])
    west = west + jnp.where(tile_row == 0, row[...], 0.0)
    east = east + jnp.where(tile_row == nt - 1, row[...], 0.0)
    return west, east, sides[0:8], sides[8:16]


def image_kernel(
    nt,
    sides,
    row,
    swapped_a,
    swapped_b,
    fields,
    probes,
    spread,
    wind,
    weights,
    costs,
    strips,
    near_row,
    far_row,
):
    west, east, south, north = outer_values(nt, sides, row, swapped_a, swapped_b)
    planes = {}
    for pp in range(3):
        u = pair(wind, (0, 0), pp)
        v = pair(wind, (1, 0), pp)
        for probe in range(PROBES):
            field = lambda n: fields[(FORWARD.index(n) * PROBES + probe) * 3 + pp]
            at = lambda n, t: (list(t).index(n) * PROBES + probe) * 3 + pp
            dx = {n: slopes_x(field(n), at(n, FORWARD_X), west, east) for n in FORWARD_X}
            dy = {n: slopes_y(field(n), at(n, FORWARD_Y), south, north) for n in FORWARD_Y}
            thickness = pair(spread, (2, 0), pp) * pair(probes, (probe, 2, 0), pp)
            z = field("zonal") - dt * (dx["geo"] + u * dx["zonal"] + v * dy["zonal"])
            m = field("meridional") - dt * (
                dy["geo"] + u * dx["meridional"] + v * dy["meridional"]
            )
            t = thickness - dt * (dx["flux_x"] + dy["flux_y"])
            h = field("temp") - dt * (u * dx["temp"] + v * dy["temp"])
            z, m, t, h = (weights[c * 3 + pp] * w for c, w in enumerate((z, m, t, h)))
            for c, w in enumerate((z, m, t, h)):
                costs[(c * PROBES + probe) * 3 + pp] = w
            made = (u * z, u * m, v * z, v * m, z, m, t, u * h, v * h)
            for n, w in zip(ADJOINT, made):
                planes[n, probe, pp] = w
    put_strips(
        [planes[n, pr, pp] for n in ADJOINT for pr in range(PROBES) for pp in range(3)],
        strips,
        lax.axis_index("tx"),
    )
    put_outer_rows(
        [planes[n, pr, pp] for n in ADJOINT_X for pr in range(PROBES) for pp in range(3)],
        near_row,
        far_row,
    )


def adjoint_kernel(
    nt,
    levels,
    sides,
    row,
    swapped_a,
    swapped_b,
    costs,
    wind,
    mass,
    heat,
    backs,
    loads,
):
    west, east, south, north = outer_values(nt, sides, row, swapped_a, swapped_b)
    for pp in range(3):
        u = pair(wind, (0, 0), pp)
        v = pair(wind, (1, 0), pp)
        mass_here = pair(mass, (0,), pp)
        heat_here = pair(heat, (0,), pp)
        for probe in range(PROBES):
            z, m, t, h = (costs[(c * PROBES + probe) * 3 + pp] for c in range(4))
            field = dict(
                zip(ADJOINT, (u * z, u * m, v * z, v * m, z, m, t, u * h, v * h))
            )
            at = lambda n, k: (list(k).index(n) * PROBES + probe) * 3 + pp
            dx = {n: slopes_x(field[n], at(n, ADJOINT_X), west, east) for n in ADJOINT_X}
            dy = {n: slopes_y(field[n], at(n, ADJOINT_Y), south, north) for n in ADJOINT_Y}
            geo_back = dt * (dx["z"] + dy["m"])
            flux_x_back = dt * dx["t"]
            flux_y_back = dt * dy["t"]
            out = (
                z + dt * (dx["ez"] + dy["nz"]) + mass_here * flux_x_back,
                m + dt * (dx["em"] + dy["nm"]) + mass_here * flux_y_back,
                t + u * flux_x_back + v * flux_y_back,
                h + dt * (dx["eh"] + dy["nh"]) + geo_back,
            )
            for c, w in enumerate(out):
                backs[(c * PROBES + probe) * 3 + pp] = w
            load = heat_here * geo_back
            for k in range(levels):
                loads[k, (probe * 3 + pp) * 8 : (probe * 3 + pp) * 8 + 8] = load


def final_kernel(level_count, probes, spread, backs, loads, out):
    level = lax.axis_index("face")
    for probe in range(PROBES):
        for pp in range(3):
            at = (probe * 3 + pp) * 8
            load = jnp.zeros((8, 128), jnp.float32)
            for k in range(level_count):
                load = load + jnp.where(k >= level, loads[k, at : at + 8], 0.0)
            for c in range(4):
                back = backs[(c * PROBES + probe) * 3 + pp]
                if c == 2:
                    back = back + load
                for side in range(2):
                    part = back[:, 64 * side : 64 * side + 64]
                    p = 2 * pp + side
                    out[probe, c, 0, p] = probes[probe, c, 0, p] + spread[c, 0, p] * part


SMEM = pl.BlockSpec(memory_space=pltpu.SMEM)
VMEM = pl.BlockSpec(memory_space=pltpu.VMEM)
INTERPRET = False
GRANT = 8 << 20


def call(kernel, operands, shapes):
    shapes = [jax.ShapeDtypeStruct(s, jnp.float32) for s in shapes]
    return pl.pallas_call(
        kernel,
        out_shape=shapes,
        in_specs=[VMEM] * len(operands),
        out_specs=[VMEM] * len(shapes),
        compiler_params=pltpu.CompilerParams(vmem_limit_bytes=GRANT),
        interpret=INTERPRET,
    )(*operands)


def thickness_copies(slots, links, probes, spread):
    return pl.pallas_call(
        functools.partial(thickness_kernel, slots),
        name="thickness",
        grid=(1,),
        out_shape=[
            jax.ShapeDtypeStruct((slots, 48, 128), jnp.float32),
            jax.ShapeDtypeStruct((4, 8, 64), jnp.float32),
        ],
        in_specs=[
            SMEM,
            pl.BlockSpec((PROBES, 1, 1, 6, 8, 64), lambda i: (0, 2, 0, 0, 0, 0)),
            pl.BlockSpec((1, 1, 6, 8, 64), lambda i: (2, 0, 0, 0, 0)),
        ],
        out_specs=[
            pl.BlockSpec((slots, 48, 128), lambda i: (0, 0, 0)),
            pl.BlockSpec((4, 8, 64), lambda i: (0, 0, 0)),
        ],
        interpret=INTERPRET,
    )(links, probes, spread)


def exchange(kind, nt, nq, table, strips, near_row, far_row):
    sources, x_targets, y_targets = TABLES[kind]
    codes = jnp.asarray(codes_of(sources, x_targets, y_targets))
    picks = jnp.asarray(picks_of(sources, y_targets))
    near = [(i, i ^ 1) for i in range(nt)]
    wrapped = [(i, (i + 1 if i % 2 else i - 1) % nt) for i in range(nt)]
    gathered = lax.all_gather(strips, "ty", axis=0)
    (slots,) = call(
        functools.partial(slots_kernel, nt, nq), (table, gathered, codes), ((nt, 8, 128),)
    )
    arrived = lax.all_to_all(slots, "tx", 0, 0, tiled=True)
    swap_b, local, halos = call(
        functools.partial(rows_kernel, nt, nq),
        (table, gathered, far_row, codes, picks),
        ((32, 128), (32, 128), (16, 64)),
    )
    swapped_b = lax.ppermute(swap_b, "tx", wrapped)
    swapped_a = lax.ppermute(near_row, "tx", near)
    sides, row = call(
        functools.partial(collect_kernel, nt, nq),
        (table, arrived, local, halos),
        ((16, 128), (32, 128)),
    )
    return sides, row, swapped_a, swapped_b


def body(probes, wind, mass, heat, spread, misfit, links):
    nf, nt, nq = (lax.axis_size(a) for a in ("face", "tx", "ty"))
    sent, table = thickness_copies(nf, links, probes, spread)
    totals = lax.all_to_all(sent, "face", 0, 0, tiled=True)
    fields, strips, *rows, weights = call(
        functools.partial(fields_kernel, nf),
        (probes, spread, wind, mass, heat, misfit, totals),
        ((36, 8, 128), (STRIP, 128), (32, 128), (32, 128), (12, 8, 128)),
    )
    outer = exchange("forward", nt, nq, table, strips, *rows)
    costs, strips, *rows = call(
        functools.partial(image_kernel, nt),
        (*outer, fields, probes, spread, wind, weights),
        ((24, 8, 128), (STRIP, 128), (32, 128), (32, 128)),
    )
    outer = exchange("adjoint", nt, nq, table, strips, *rows)
    backs, loads = call(
        functools.partial(adjoint_kernel, nt, nf),
        (*outer, costs, wind, mass, heat),
        ((24, 8, 128), (nf, 48, 128)),
    )
    loads = lax.all_to_all(loads, "face", 0, 0, tiled=True)
    (applied,) = call(
        functools.partial(final_kernel, nf), (probes, spread, backs, loads), (probes.shape,)
    )
    return applied


def solution(mesh):
    return jax.shard_map(
        body,
        mesh=mesh,
        in_specs=(
            P(None, None, "face", None, "tx", "ty"),
            P(None, "face", None, "tx", "ty"),
            P("face", None, "tx", "ty"),
            P("face", None, "tx", "ty"),
            P(None, "face", None, "tx", "ty"),
            P(None, "face", None, "tx", "ty"),
            P(),
        ),
        out_specs=P(None, None, "face", None, "tx", "ty"),
        check_vma=False,
    )
```
